256 devices in a mesh: seq: 32 (over z, x), tp: 8 (over y, core).
Axes of the slice: x: 4, y: 4, z: 8, core: 2. Of those that a mesh axis runs over, the one named last changes fastest.
Arguments:
- queries: bfloat16 [8192, 8192], P('seq', 'tp'), may hold values from -120 to 120
- keys: bfloat16 [8192, 1024], P('seq', 'tp'), may hold values from -5 to 5
- values: bfloat16 [8192, 1024], P('seq', 'tp'), may hold values from -6 to 6
- w_query: bfloat16 [8192, 8192], P('seq', 'tp'), may hold values from -0.0625 to 0.0625
- key_weight: bfloat16 [8192, 1024], P('seq'), may hold values from -0.0625 to 0.0625
Outputs:
- attended: bfloat16 [8192, 8192], P('seq', 'tp')
- head_logit_maxima: float32 [64], P('tp')
- w_query_clipped: bfloat16 [8192, 8192], P('seq', 'tp')
- clipped_key_weight: bfloat16 [8192, 1024], P('seq')
The draws below stay inside these ranges and needn't reach their ends.
All inputs are finite; a program needn't handle non-finite values.
Results may differ from the reference program's by a relative error of at most 0.004.
Values may be sent and summed in bfloat16 or wider, within the bound.
No kernel may reach another device: no remote copies, remote signals or barrier semaphores. Data moves between devices by JAX's collectives and lax.ppermute only.
A program may use at most 64 MiB of HBM per device.

```python
import math
import jax
import jax.numpy as jnp
from jax import lax

MODEL_WIDTH = 8192
QUERY_HEADS = 64
KEY_VALUE_HEADS = 8
HEAD_SIZE = 128
SEQUENCE_LENGTH = 8192


def random_key_table(key):
    gaussian_sample = jnp.clip(jax.random.normal(jax.random.fold_in(key, 71), (SEQUENCE_LENGTH, KEY_VALUE_HEADS, HEAD_SIZE), jnp.float32), -5.0, 5.0)
    return gaussian_sample


def draw_keys(key, part):
    return random_key_table(key).reshape(SEQUENCE_LENGTH, KEY_VALUE_HEADS * HEAD_SIZE).astype(jnp.bfloat16)


def draw_queries(key, part):
    head_scale = jnp.exp(jax.random.uniform(jax.random.fold_in(key, 72), (QUERY_HEADS,), jnp.float32, math.log(0.3), math.log(3.0)))
    gaussian_sample = jnp.clip(jax.random.normal(jax.random.fold_in(key, 73), (SEQUENCE_LENGTH, QUERY_HEADS, HEAD_SIZE), jnp.float32), -5.0, 5.0)
    gaussian_sample = gaussian_sample * head_scale[None, :, None]
    return gaussian_sample.reshape(SEQUENCE_LENGTH, QUERY_HEADS * HEAD_SIZE).astype(jnp.bfloat16)


def levels(rng, dims, shards, least, top_value):
    loudness = 1.0
    for position, parts in shards:
        draws = jax.random.uniform(jax.random.fold_in(jax.random.fold_in(rng, 6), position), (parts,), jnp.float32, least / len(shards), top_value / len(shards))
        loudness = loudness * jnp.repeat(jnp.exp(draws), dims[position] // parts).reshape((-1,) + (1,) * (len(dims) - 1 - position))
    return loudness


def centred(own_key, dims, width, bound, pieces=(), held_as=jnp.bfloat16):
    factor_of = levels(own_key, dims, pieces, -0.22, 0.18) if pieces else 1.0
    values = jax.random.normal(own_key, dims, jnp.float32) * width * factor_of
    return jnp.minimum(jnp.maximum(values, -bound), bound).astype(held_as)


def setup_inputs(seed: int = 0) -> dict:
    arg_keys = jax.random.split(jax.random.key(seed), 6)
    return {
        "queries": draw_queries(jax.random.fold_in(arg_keys[5], 71), 0),
        "keys": draw_keys(jax.random.fold_in(arg_keys[5], 71), 0),
        "values": centred(arg_keys[2], (SEQUENCE_LENGTH, KEY_VALUE_HEADS * HEAD_SIZE), 1.0, 6.0, ((0, 32), (1, 8))),
        "w_query": centred(arg_keys[3], (MODEL_WIDTH, QUERY_HEADS * HEAD_SIZE), MODEL_WIDTH ** -0.5, 0.0625, ((0, 32), (1, 8))),
        "key_weight": centred(arg_keys[4], (MODEL_WIDTH, KEY_VALUE_HEADS * HEAD_SIZE), MODEL_WIDTH ** -0.5, 0.0625, ((0, 32),)),
    }


clip_threshold = 10.0

def reference(queries, keys, values, w_query, key_weight):
    group_size = QUERY_HEADS // KEY_VALUE_HEADS
    block_rows = math.gcd(SEQUENCE_LENGTH, 512)
    inv_sqrt = HEAD_SIZE ** (-0.5)
    query_heads_view = jnp.moveaxis(queries.reshape(SEQUENCE_LENGTH, KEY_VALUE_HEADS, group_size, HEAD_SIZE), 1, 0)
    key_heads_view = jnp.moveaxis(keys.reshape(SEQUENCE_LENGTH, KEY_VALUE_HEADS, HEAD_SIZE), 1, 0)
    value_heads_view = jnp.moveaxis(values.reshape(SEQUENCE_LENGTH, KEY_VALUE_HEADS, HEAD_SIZE), 1, 0)
    key_positions = jnp.arange(SEQUENCE_LENGTH, dtype=jnp.int32)

    def one_head(operands):
        head_queries, head_keys, head_values = operands
        keys_wide = head_keys.astype(jnp.float32)
        values_wide = head_values.astype(jnp.float32)

        def one_block(running, block_index):
            block_queries = lax.dynamic_slice_in_dim(head_queries, block_index * block_rows, block_rows, 0).astype(jnp.float32)
            scores = jnp.einsum('bgd,nd->bgn', block_queries, keys_wide) * inv_sqrt
            query_positions = block_index * block_rows + jnp.arange(block_rows, dtype=jnp.int32)
            visible = (query_positions[:, None] >= key_positions[None, :])[:, None, :]
            masked = jnp.where(visible, scores, jnp.float32(-1e+30))
            row_max = masked.max(-1)
            expo = jnp.where(visible, jnp.exp(masked - row_max[..., None]), jnp.float32(0.0))
            totals = expo.sum(-1)
            probs = lax.optimization_barrier(expo.astype(jnp.bfloat16)).astype(jnp.float32)
            mixed = jnp.einsum('bgn,nd->bgd', probs, values_wide) / totals[..., None]
            return (jnp.maximum(running, masked.max(axis=(0, 2))), mixed.astype(jnp.bfloat16))
        head_max, block_out = lax.scan(one_block, jnp.full((group_size,), -1e+30, jnp.float32), jnp.arange(SEQUENCE_LENGTH // block_rows, dtype=jnp.int32))
        return (head_max, block_out.reshape(SEQUENCE_LENGTH, group_size, HEAD_SIZE))
    head_max, outputs = lax.map(one_head, (query_heads_view, key_heads_view, value_heads_view))
    attended = jnp.moveaxis(outputs, 0, 1).reshape(SEQUENCE_LENGTH, QUERY_HEADS * HEAD_SIZE)
    head_logit_maxima = head_max.reshape(QUERY_HEADS)
    gamma = clip_threshold / jnp.maximum(head_logit_maxima, clip_threshold)
    clip_logits = clip_threshold / jnp.maximum(head_logit_maxima.reshape(KEY_VALUE_HEADS, group_size).max(1), clip_threshold)
    query_factor = gamma / jnp.sqrt(jnp.repeat(clip_logits, group_size))
    w_query_clipped = (w_query.astype(jnp.float32).reshape(MODEL_WIDTH, QUERY_HEADS, HEAD_SIZE) * query_factor[None, :, None]).reshape(MODEL_WIDTH, QUERY_HEADS * HEAD_SIZE).astype(jnp.bfloat16)
    clipped_key_weight = (key_weight.astype(jnp.float32).reshape(MODEL_WIDTH, KEY_VALUE_HEADS, HEAD_SIZE) * jnp.sqrt(clip_logits)[None, :, None]).reshape(MODEL_WIDTH, KEY_VALUE_HEADS * HEAD_SIZE).astype(jnp.bfloat16)
    return (attended, head_logit_maxima, w_query_clipped, clipped_key_weight)
```

```python
import jax
import jax.numpy as jnp
from jax import lax
from jax.experimental import pallas as pl
from jax.experimental.pallas import tpu as pltpu
from jax.sharding import PartitionSpec as P

HEAD_SIZE = 128
CLIP_THRESHOLD = 10.0
LOG2E = 1.4426950408889634
SCALE = HEAD_SIZE**-0.5 * LOG2E
LARGEST_STEP = 100.0
LOW = -1e30
X = 4
PIECE = 128


NT = (((1,), (1,)), ((), ()))


def dot_nt(a, b):
    return lax.dot_general(a, b, NT, preferred_element_type=jnp.float32)


def scaled_queries(q):
    exact = q.astype(jnp.float32) * SCALE
    high = exact.astype(jnp.bfloat16)
    low = (exact - high.astype(jnp.float32)).astype(jnp.bfloat16)
    return jnp.concatenate([high, low], axis=1)


def with_ones(v):
    return jnp.concatenate([v, jnp.ones_like(v)], axis=1)


def across(column, width):
    return jnp.tile(column, (1, width // column.shape[1]))


def by_sublane(a):
    out = a[:8]
    for r in range(8, a.shape[0], 8):
        out = jnp.maximum(out, a[r : r + 8])
    return out


def own_kernel(heads, q_ref, kv_ref, m_ref, l_ref, a_ref, hm_ref):
    rows = q_ref.shape[0]
    k = kv_ref[:, :HEAD_SIZE]
    kk = jnp.concatenate([k, k], axis=1)
    ve = with_ones(kv_ref[:, HEAD_SIZE:])
    seen = lax.broadcasted_iota(jnp.int32, (rows, rows), 0) >= lax.broadcasted_iota(
        jnp.int32, (rows, rows), 1
    )
    for h in range(heads):
        q = scaled_queries(q_ref[:, h * HEAD_SIZE : (h + 1) * HEAD_SIZE])
        s = jnp.where(seen, dot_nt(q, kk), LOW)
        m = jnp.broadcast_to(jnp.max(s, axis=1, keepdims=True), (rows, HEAD_SIZE))
        p = jnp.exp2(s - across(m, rows)).astype(jnp.bfloat16)
        o = jnp.dot(p, ve, preferred_element_type=jnp.float32)
        m_ref[h] = m
        a_ref[h] = o[:, :HEAD_SIZE]
        l_ref[h] = o[:, HEAD_SIZE:]
        hm_ref[h] = by_sublane(m)


def more_kernel(heads, sources, counts, last, at_ref, q_ref, own_ref, *refs):
    n = len(counts)
    pieces, refs = refs[:n], refs[n:]
    if last:
        (m_in, l_in, a_in, hm_in, out_ref, hm_out, kk, ve, m_ref, l_ref, a_ref) = refs
    else:
        (m_in, l_in, a_in, hm_in, m_ref, l_ref, a_ref, hm_out, kk, ve) = refs
    rows = q_ref.shape[0]
    total = sum(counts)
    place = at_ref[0]
    z, x = place // X, place % X
    first_key = jnp.broadcast_to(own_ref[0:1, :HEAD_SIZE], (PIECE, HEAD_SIZE))
    base = 0
    for ref, count, source in zip(pieces, counts, sources):
        for i in range(0, count, PIECE):
            dz, dx, zs = source[i // PIECE]
            came_from = lax.rem(z + zs - dz, zs) * X + lax.rem(x + X - dx, X)
            earlier = came_from < place
            k = jnp.where(earlier, ref[i : i + PIECE, :HEAD_SIZE], first_key)
            v = ref[i : i + PIECE, HEAD_SIZE:]
            at = pl.ds(base + i, PIECE)
            kk[at, :HEAD_SIZE] = k
            kk[at, HEAD_SIZE:] = k
            ve[at, :HEAD_SIZE] = jnp.where(earlier, v, jnp.zeros_like(v))
            ve[at, HEAD_SIZE:] = jnp.where(earlier, jnp.ones_like(v), jnp.zeros_like(v))
        base += count

    tiles, at = [], 0
    while at < total:
        size = min(1024, total - at)
        tiles.append((at, size))
        at += size

    def queries(h):
        return scaled_queries(q_ref[:, pl.ds(h * HEAD_SIZE, HEAD_SIZE)])

    def put(h, m, l, a, top):
        if last:
            out_ref[:, pl.ds(h * HEAD_SIZE, HEAD_SIZE)] = (a / l).astype(out_ref.dtype)
        else:
            l_ref[h] = l
            a_ref[h] = a
            m_ref[h] = m
        hm_out[h] = jnp.maximum(hm_in[h], top)

    largest = jnp.full((8, HEAD_SIZE), LOW, jnp.float32)
    for h in range(heads):
        q = queries(h)
        m = m_in[h]
        step = jnp.full((rows, HEAD_SIZE), LOW, jnp.float32)
        o = None
        for start, size in tiles:
            d = dot_nt(q, kk[start : start + size]) - across(m, size)
            for j in range(0, size, HEAD_SIZE):
                step = jnp.maximum(step, d[:, j : j + HEAD_SIZE])
            p = jnp.exp2(d).astype(jnp.bfloat16)
            pv = jnp.dot(p, ve[start : start + size], preferred_element_type=jnp.float32)
            o = pv if o is None else o + pv
        largest = jnp.maximum(largest, by_sublane(step))
        put(h, m, l_in[h] + o[:, HEAD_SIZE:], a_in[h] + o[:, :HEAD_SIZE], by_sublane(step + m))

    @pl.when(jnp.max(largest) > LARGEST_STEP)
    def _():
        def again(h, carry):
            h = jnp.int32(h)
            q = scaled_queries(q_ref[:, pl.ds(pl.multiple_of(h * HEAD_SIZE, HEAD_SIZE), HEAD_SIZE)])

            def tile(i, state):
                m, l, a = state
                at = pl.ds(pl.multiple_of(i * PIECE, PIECE), PIECE)
                s = dot_nt(q, kk[at])
                new = jnp.maximum(m, jnp.broadcast_to(jnp.max(s, axis=1, keepdims=True), m.shape))
                p = jnp.exp2(s - new).astype(jnp.bfloat16)
                o = jnp.dot(p, ve[at], preferred_element_type=jnp.float32)
                keep = jnp.exp2(m - new)
                return new, l * keep + o[:, HEAD_SIZE:], a * keep + o[:, :HEAD_SIZE]

            m, l, a = lax.fori_loop(0, total // PIECE, tile, (m_in[h], l_in[h], a_in[h]))
            if last:
                out_ref[:, pl.ds(pl.multiple_of(h * HEAD_SIZE, HEAD_SIZE), HEAD_SIZE)] = (a / l).astype(
                    out_ref.dtype
                )
            else:
                m_ref[h] = m
                l_ref[h] = l
                a_ref[h] = a
            hm_out[h] = jnp.maximum(hm_in[h], by_sublane(m))
            return carry

        lax.fori_loop(0, heads, again, 0)


VMEM = pl.BlockSpec(memory_space=pltpu.VMEM)
SMEM = pl.BlockSpec(memory_space=pltpu.SMEM)


def state_types(heads, rows):
    wide = jax.ShapeDtypeStruct((heads, rows, HEAD_SIZE), jnp.float32)
    return [wide, wide, wide, jax.ShapeDtypeStruct((heads, 8, HEAD_SIZE), jnp.float32)]


def cost(rows, heads, keys):
    return pl.CostEstimate(
        flops=4 * rows * heads * keys * HEAD_SIZE,
        bytes_accessed=2 * rows * heads * HEAD_SIZE,
        transcendentals=rows * heads * keys,
    )


def attend_own(q, kv, heads):
    rows = q.shape[0]
    return pl.pallas_call(
        lambda *refs: own_kernel(heads, *refs),
        out_shape=state_types(heads, rows),
        in_specs=[VMEM, VMEM],
        out_specs=[VMEM] * 4,
        compiler_params=pltpu.CompilerParams(vmem_limit_bytes=40 << 20),
        cost_estimate=cost(rows, heads, rows),
        name="attend_own",
    )(q, kv)


def attend_more(at, q, kv, pieces, sources, state, heads, name, last=False):
    rows = q.shape[0]
    counts = [p.shape[0] for p in pieces]
    total = sum(counts)
    types = state_types(heads, rows)
    scratch = [pltpu.VMEM((total, 2 * HEAD_SIZE), jnp.bfloat16)] * 2
    if last:
        out_shape = [jax.ShapeDtypeStruct(q.shape, jnp.bfloat16), types[3]]
        scratch += [pltpu.VMEM((8, HEAD_SIZE), jnp.float32)] * 3
    else:
        out_shape = types
    return pl.pallas_call(
        lambda *refs: more_kernel(heads, sources, counts, last, *refs),
        out_shape=out_shape,
        in_specs=[SMEM] + [VMEM] * (2 + len(pieces) + 4),
        out_specs=[VMEM] * len(out_shape),
        scratch_shapes=scratch,
        compiler_params=pltpu.CompilerParams(vmem_limit_bytes=40 << 20),
        cost_estimate=cost(rows, heads, total),
        name=name,
    )(at, q, kv, *pieces, *state)


def shards(queries, keys, values, w_query, key_weight):
    heads = queries.shape[1] // HEAD_SIZE
    seq_size, tp_size = lax.axis_size("seq"), lax.axis_size("tp")
    zs = seq_size // X
    place = lax.axis_index("seq")
    at = place.reshape(1).astype(jnp.int32)

    def moved(a, dz, dx):
        pairs = [
            (z * X + x, ((z + dz) % zs) * X + (x + dx) % X) for z in range(zs) for x in range(X)
        ]
        return lax.ppermute(a, "seq", pairs)

    kv = jnp.concatenate([keys, values], axis=1)
    half_a, half_b = kv[:PIECE], kv[PIECE:]
    state = attend_own(queries, kv, heads)

    up, down, b_x = [half_a], [half_a], {}
    for dx in (1, 3, 2):
        b_x[dx] = moved(half_b, 0, dx)
    up.append(moved(up[-1], 1, 0))
    down.append(moved(down[-1], zs - 1, 0))
    b_layer = jnp.concatenate([half_b, b_x[1], b_x[2], b_x[3]], axis=0)
    b_up, b_down = [b_layer], [b_layer]
    up.append(moved(up[-1], 1, 0))
    down.append(moved(down[-1], zs - 1, 0))
    b_up.append(moved(b_up[-1], 1, 0))
    b_down.append(moved(b_down[-1], zs - 1, 0))
    near = jnp.concatenate([half_a, up[1], down[1], up[2]], axis=0)
    near_x = {dx: moved(near, 0, dx) for dx in (1, 3, 2)}
    up.append(moved(up[-1], 1, 0))
    down.append(moved(down[-1], zs - 1, 0))
    b_up.append(moved(b_up[-1], 1, 0))
    b_down.append(moved(b_down[-1], zs - 1, 0))
    up.append(moved(up[-1], 1, 0))
    b_up.append(moved(b_up[-1], 1, 0))
    b_down.append(moved(b_down[-1], zs - 1, 0))
    far = jnp.concatenate([down[2], up[3], down[3], up[4]], axis=0)
    far_x = {dx: moved(far, 0, dx) for dx in (1, 3, 2)}
    b_up.append(moved(b_up[-1], 1, 0))

    def column(dz, dx=0):
        return (dz % zs, dx, zs)

    near_z, far_z, layer = (0, 1, -1, 2), (-2, 3, -3, 4), (0, 1, 2, 3)

    def more(state, name, parts, last=False):
        pieces, sources = zip(*parts)
        return attend_more(at, queries, kv, pieces, sources, state, heads, name, last)

    def b_part(k):
        return (b_up[k] if k > 0 else b_down[-k], [column(k, dx) for dx in layer])

    def x_part(held, zlist):
        return [(held[dx], [column(k, dx) for k in zlist]) for dx in (1, 2, 3)]

    state = more(
        state,
        "attend_1",
        [(b_x[dx], [column(0, dx)]) for dx in (1, 2, 3)]
        + [(up[k], [column(k)]) for k in (1, 2, 3, 4)]
        + [(down[k], [column(-k)]) for k in (1, 2, 3)],
    )
    state = more(state, "attend_2", [b_part(1), b_part(-1)])
    state = more(state, "attend_3", x_part(near_x, near_z))
    state = more(state, "attend_4", [b_part(2), b_part(-2)])
    state = more(state, "attend_5", [b_part(3), b_part(-3)])
    state = more(state, "attend_6", x_part(far_x, far_z))
    attended, head_top = more(state, "attend_7", [b_part(4)], last=True)

    local_max = jnp.max(head_top, axis=(1, 2)) * jnp.float32(1.0 / LOG2E)
    devices = seq_size * tp_size
    everyones = lax.all_to_all(
        jnp.broadcast_to(local_max[None], (devices, heads)), ("seq", "tp"), 0, 0, tiled=True
    )
    all_maxima = jnp.max(everyones.reshape(seq_size, tp_size, heads), axis=0)
    head_max = lax.dynamic_index_in_dim(all_maxima, lax.axis_index("tp"), 0, keepdims=False)
    group_clip = CLIP_THRESHOLD / jnp.maximum(all_maxima.max(1), CLIP_THRESHOLD)
    own_clip = CLIP_THRESHOLD / jnp.maximum(head_max.max(), CLIP_THRESHOLD)
    gamma = CLIP_THRESHOLD / jnp.maximum(head_max, CLIP_THRESHOLD)
    query_factor = gamma / jnp.sqrt(own_clip)

    def scaled(weight, factors):
        rows, columns = weight.shape
        wide = jnp.broadcast_to(factors[:, None], (factors.shape[0], HEAD_SIZE)).reshape(1, columns)
        return (weight.astype(jnp.float32) * wide).astype(jnp.bfloat16)

    return (
        attended,
        head_max,
        scaled(w_query, query_factor),
        scaled(key_weight, jnp.sqrt(group_clip)),
    )


def solution(mesh):
    in_specs = (P("seq", "tp"), P("seq", "tp"), P("seq", "tp"), P("seq", "tp"), P("seq", None))
    out_specs = (P("seq", "tp"), P("tp"), P("seq", "tp"), P("seq", None))
    return jax.shard_map(shards, mesh=mesh, in_specs=in_specs, out_specs=out_specs, check_vma=False)
```

```python
import jax
import jax.numpy as jnp
from jax import lax
from jax.experimental import pallas as pl
from jax.experimental.pallas import tpu as pltpu
from jax.sharding import PartitionSpec as P

HEAD_SIZE = 128
CLIP_THRESHOLD = 10.0
LOG2E = 1.4426950408889634
SCALE = HEAD_SIZE**-0.5 * LOG2E
LARGEST_STEP = 100.0
LOW = -1e30
X = 4
A_ROWS = 128
HEADS_AT_ONCE = 4


NT = (((1,), (1,)), ((), ()))


def dot_nt(a, b):
    return lax.dot_general(a, b, NT, preferred_element_type=jnp.float32)


def scaled_queries(q):
    exact = q.astype(jnp.float32) * SCALE
    high = exact.astype(jnp.bfloat16)
    low = (exact - high.astype(jnp.float32)).astype(jnp.bfloat16)
    return jnp.concatenate([high, low], axis=1)


def with_ones(v):
    return jnp.concatenate([v, jnp.ones_like(v)], axis=1)


def across(column, width):
    return jnp.tile(column, (1, width // column.shape[1]))


def by_sublane(a):
    out = a[:8]
    for r in range(8, a.shape[0], 8):
        out = jnp.maximum(out, a[r : r + 8])
    return out


def own_kernel(heads, q_ref, kv_ref, m_ref, l_ref, a_ref, hm_ref):
    rows = q_ref.shape[0]
    k = kv_ref[:, :HEAD_SIZE]
    kk = jnp.concatenate([k, k], axis=1)
    ve = with_ones(kv_ref[:, HEAD_SIZE:])
    seen = lax.broadcasted_iota(jnp.int32, (rows, rows), 0) >= lax.broadcasted_iota(
        jnp.int32, (rows, rows), 1
    )
    for h in range(heads):
        q = scaled_queries(q_ref[:, h * HEAD_SIZE : (h + 1) * HEAD_SIZE])
        s = jnp.where(seen, dot_nt(q, kk), LOW)
        m = jnp.broadcast_to(jnp.max(s, axis=1, keepdims=True), (rows, HEAD_SIZE))
        p = jnp.exp2(s - across(m, rows)).astype(jnp.bfloat16)
        o = jnp.dot(p, ve, preferred_element_type=jnp.float32)
        m_ref[h] = m
        a_ref[h] = o[:, :HEAD_SIZE]
        l_ref[h] = o[:, HEAD_SIZE:]
        hm_ref[h] = by_sublane(m)


def more_kernel(heads, sources, counts, last, at_ref, q_ref, own_ref, *refs):
    n = len(counts)
    pieces, refs = refs[:n], refs[n:]
    if last:
        (m_in, l_in, a_in, hm_in, out_ref, hm_out, kk, ve) = refs
    else:
        (m_in, l_in, a_in, hm_in, m_ref, l_ref, a_ref, hm_out, kk, ve) = refs
    rows = q_ref.shape[0]
    total = sum(counts)
    place = at_ref[0]
    z, x = place // X, place % X
    base, visible = 0, []
    for ref, count, source in zip(pieces, counts, sources):
        size = count // len(source)
        for i, (dz, dx, zs) in enumerate(source):
            came_from = lax.rem(z + zs - dz, zs) * X + lax.rem(x + X - dx, X)
            visible.append((ref, i * size, base, size, came_from < place))
            base += size
    some = visible[0][-1]
    for piece in visible[1:]:
        some = jnp.logical_or(some, piece[-1])

    tiles, at = [], 0
    while at < total:
        size = min(1024, total - at)
        tiles.append((at, size))
        at += size

    def columns(h):
        return pl.ds(pl.multiple_of(h * HEAD_SIZE, HEAD_SIZE), HEAD_SIZE)

    def put(h, m, l, a, top):
        if last:
            out_ref[:, columns(h)] = (a / l).astype(out_ref.dtype)
        else:
            l_ref[h] = l
            a_ref[h] = a
            m_ref[h] = m
        hm_out[h] = jnp.maximum(hm_in[h], top)

    def per_head(body, first):
        def some_heads(i, carry):
            for j in range(HEADS_AT_ONCE):
                carry = body(i * HEADS_AT_ONCE + j, carry)
            return carry

        return lax.fori_loop(0, heads // HEADS_AT_ONCE, some_heads, first)

    @pl.when(jnp.logical_not(some))
    def _():
        def unchanged(h, carry):
            put(h, m_in[h], l_in[h], a_in[h], hm_in[h])
            return carry

        lax.fori_loop(0, heads, unchanged, 0)

    @pl.when(some)
    def _():
        first_key = own_ref[0:1, :HEAD_SIZE]
        for ref, start, base, size, earlier in visible:
            k = jnp.where(
                earlier,
                ref[start : start + size, :HEAD_SIZE],
                jnp.broadcast_to(first_key, (size, HEAD_SIZE)),
            )
            v = ref[start : start + size, HEAD_SIZE:]
            at = pl.ds(base, size)
            kk[at, :HEAD_SIZE] = k
            kk[at, HEAD_SIZE:] = k
            ve[at, :HEAD_SIZE] = jnp.where(earlier, v, jnp.zeros_like(v))
            ve[at, HEAD_SIZE:] = jnp.where(earlier, jnp.ones_like(v), jnp.zeros_like(v))

        def head(h, largest):
            q = scaled_queries(q_ref[:, columns(h)])
            m = m_in[h]
            step = jnp.full((rows, HEAD_SIZE), LOW, jnp.float32)
            o = None
            for start, size in tiles:
                d = dot_nt(q, kk[start : start + size]) - across(m, size)
                for j in range(0, size, HEAD_SIZE):
                    step = jnp.maximum(step, d[:, j : j + HEAD_SIZE])
                p = jnp.exp2(d).astype(jnp.bfloat16)
                pv = jnp.dot(p, ve[start : start + size], preferred_element_type=jnp.float32)
                o = pv if o is None else o + pv
            put(h, m, l_in[h] + o[:, HEAD_SIZE:], a_in[h] + o[:, :HEAD_SIZE], by_sublane(step + m))
            return jnp.maximum(largest, by_sublane(step))

        largest = per_head(head, jnp.full((8, HEAD_SIZE), LOW, jnp.float32))

        @pl.when(jnp.max(largest) > LARGEST_STEP)
        def _():
            def again(h, carry):
                q = scaled_queries(q_ref[:, columns(h)])

                def tile(i, state):
                    m, l, a = state
                    at = pl.ds(pl.multiple_of(i * HEAD_SIZE, HEAD_SIZE), HEAD_SIZE)
                    s = dot_nt(q, kk[at])
                    new = jnp.maximum(m, jnp.broadcast_to(jnp.max(s, axis=1, keepdims=True), m.shape))
                    p = jnp.exp2(s - new).astype(jnp.bfloat16)
                    o = jnp.dot(p, ve[at], preferred_element_type=jnp.float32)
                    keep = jnp.exp2(m - new)
                    return new, l * keep + o[:, HEAD_SIZE:], a * keep + o[:, :HEAD_SIZE]

                m, l, a = lax.fori_loop(0, total // HEAD_SIZE, tile, (m_in[h], l_in[h], a_in[h]))
                put(h, m, l, a, by_sublane(m))
                return carry

            lax.fori_loop(0, heads, again, 0)


VMEM = pl.BlockSpec(memory_space=pltpu.VMEM)
SMEM = pl.BlockSpec(memory_space=pltpu.SMEM)


def state_types(heads, rows):
    wide = jax.ShapeDtypeStruct((heads, rows, HEAD_SIZE), jnp.float32)
    return [wide, wide, wide, jax.ShapeDtypeStruct((heads, 8, HEAD_SIZE), jnp.float32)]


def cost(rows, heads, keys):
    return pl.CostEstimate(
        flops=4 * rows * heads * keys * HEAD_SIZE,
        bytes_accessed=2 * rows * heads * HEAD_SIZE,
        transcendentals=rows * heads * keys,
    )


def attend_own(q, kv, heads):
    rows = q.shape[0]
    return pl.pallas_call(
        lambda *refs: own_kernel(heads, *refs),
        out_shape=state_types(heads, rows),
        in_specs=[VMEM, VMEM],
        out_specs=[VMEM] * 4,
        compiler_params=pltpu.CompilerParams(vmem_limit_bytes=40 << 20),
        cost_estimate=cost(rows, heads, rows),
        name="attend_own",
    )(q, kv)


def attend_more(at, q, kv, pieces, sources, state, heads, name, last=False):
    rows = q.shape[0]
    counts = [p.shape[0] for p in pieces]
    total = sum(counts)
    types = state_types(heads, rows)
    scratch = [pltpu.VMEM((total, 2 * HEAD_SIZE), jnp.bfloat16)] * 2
    if last:
        out_shape = [jax.ShapeDtypeStruct(q.shape, jnp.bfloat16), types[3]]
    else:
        out_shape = types
    return pl.pallas_call(
        lambda *refs: more_kernel(heads, sources, counts, last, *refs),
        out_shape=out_shape,
        in_specs=[SMEM] + [VMEM] * (2 + len(pieces) + 4),
        out_specs=[VMEM] * len(out_shape),
        scratch_shapes=scratch,
        compiler_params=pltpu.CompilerParams(vmem_limit_bytes=40 << 20),
        cost_estimate=cost(rows, heads, total),
        name=name,
    )(at, q, kv, *pieces, *state)


def shards(queries, keys, values, w_query, key_weight):
    heads = queries.shape[1] // HEAD_SIZE
    seq_size, tp_size = lax.axis_size("seq"), lax.axis_size("tp")
    zs = seq_size // X
    place = lax.axis_index("seq")
    at = place.reshape(1).astype(jnp.int32)

    def moved(a, dz, dx, wanted):
        pairs = [
            (((z - dz) % zs) * X + (x - dx) % X, z * X + x)
            for z in range(zs)
            for x in range(X)
            if wanted(z, x)
        ]
        return lax.ppermute(a, "seq", pairs)

    def earlier(dz, dx=0):
        return lambda z, x: ((z - dz) % zs, (x - dx) % X) < (z, x)

    def any_earlier(dzs, dx):
        return lambda z, x: any(earlier(dz, dx)(z, x) for dz in dzs)

    def down_wanted(j):
        return lambda z, x: any((z - i) % zs + j + i >= zs for i in range(furthest_down - j + 1))

    furthest_down = zs // 2 - 1
    kv = jnp.concatenate([keys, values], axis=1)
    half_a, half_b = kv[:A_ROWS], kv[A_ROWS:]
    state = attend_own(queries, kv, heads)

    b_x = {
        dx: moved(half_b, 0, dx, lambda z, x: z < zs - 1 or earlier(0, dx)(z, x)) for dx in (1, 3, 2)
    }
    col = {dz: moved(half_a, dz, 0, earlier(dz)) for dz in (1, -1, 2, -2, 3, -3, 4)}
    layer = jnp.concatenate([half_b, b_x[1], b_x[2], b_x[3]], axis=0)
    b_up, b_down = [layer], [layer]
    for k in range(1, zs // 2 + 1):
        b_up.append(moved(b_up[-1], 1, 0, earlier(k)))
        if k <= furthest_down:
            b_down.append(moved(b_down[-1], -1, 0, down_wanted(k)))
    near_z, far_z, around = (0, 1, -1, 2), (-2, 3, -3, 4), (0, 1, 2, 3)
    near = jnp.concatenate([half_a] + [col[dz] for dz in near_z[1:]], axis=0)
    near_x = {dx: moved(near, 0, dx, any_earlier(near_z, dx)) for dx in (1, 3, 2)}
    far = jnp.concatenate([col[dz] for dz in far_z], axis=0)
    far_x = {dx: moved(far, 0, dx, any_earlier(far_z, dx)) for dx in (1, 3, 2)}

    def source(dz, dx=0):
        return (dz % zs, dx, zs)

    def more(state, name, parts, last=False):
        pieces, sources = zip(*parts)
        return attend_more(at, queries, kv, pieces, sources, state, heads, name, last)

    def b_part(k):
        return (b_up[k] if k > 0 else b_down[-k], [source(k, dx) for dx in around])

    def x_part(held, dzs):
        return [(held[dx], [source(dz, dx) for dz in dzs]) for dx in (1, 2, 3)]

    state = more(
        state,
        "attend_1",
        [(b_x[dx], [source(0, dx)]) for dx in (1, 2, 3)]
        + [(col[dz], [source(dz)]) for dz in (1, -1, 2, -2, 3, -3, 4)],
    )
    state = more(state, "attend_2", [b_part(1), b_part(-1)])
    state = more(state, "attend_3", x_part(near_x, near_z))
    state = more(state, "attend_4", [b_part(2), b_part(-2)])
    state = more(state, "attend_5", x_part(far_x, far_z))
    state = more(state, "attend_6", [b_part(3), b_part(-3)])
    attended, head_top = more(state, "attend_7", [b_part(4)], last=True)

    local_max = jnp.max(head_top, axis=(1, 2)) * jnp.float32(1.0 / LOG2E)
    devices = seq_size * tp_size
    everyones = lax.all_to_all(
        jnp.broadcast_to(local_max[None], (devices, heads)), ("seq", "tp"), 0, 0, tiled=True
    )
    all_maxima = jnp.max(everyones.reshape(seq_size, tp_size, heads), axis=0)
    head_max = lax.dynamic_index_in_dim(all_maxima, lax.axis_index("tp"), 0, keepdims=False)
    group_clip = CLIP_THRESHOLD / jnp.maximum(all_maxima.max(1), CLIP_THRESHOLD)
    own_clip = CLIP_THRESHOLD / jnp.maximum(head_max.max(), CLIP_THRESHOLD)
    gamma = CLIP_THRESHOLD / jnp.maximum(head_max, CLIP_THRESHOLD)
    query_factor = gamma / jnp.sqrt(own_clip)

    def scaled(weight, factors):
        rows, columns = weight.shape
        wide = jnp.broadcast_to(factors[:, None], (factors.shape[0], HEAD_SIZE)).reshape(1, columns)
        return (weight.astype(jnp.float32) * wide).astype(jnp.bfloat16)

    return (
        attended,
        head_max,
        scaled(w_query, query_factor),
        scaled(key_weight, jnp.sqrt(group_clip)),
    )


def solution(mesh):
    in_specs = (P("seq", "tp"), P("seq", "tp"), P("seq", "tp"), P("seq", "tp"), P("seq", None))
    out_specs = (P("seq", "tp"), P("tp"), P("seq", "tp"), P("seq", None))
    return jax.shard_map(shards, mesh=mesh, in_specs=in_specs, out_specs=out_specs, check_vma=False)
```

```python
import jax
import jax.numpy as jnp
from jax import lax
from jax.experimental import pallas as pl
from jax.experimental.pallas import tpu as pltpu
from jax.sharding import PartitionSpec as P

HEAD_SIZE = 128
CLIP_THRESHOLD = 10.0
LOG2E = 1.4426950408889634
SCALE = HEAD_SIZE**-0.5 * LOG2E
LARGEST_STEP = 100.0
LOW = -1e30
X = 4
A_ROWS = 128
HEADS_AT_ONCE = 8


NT = (((1,), (1,)), ((), ()))


def dot_nt(a, b):
    return lax.dot_general(a, b, NT, preferred_element_type=jnp.float32)


def scaled_queries(q):
    exact = q.astype(jnp.float32) * SCALE
    high = exact.astype(jnp.bfloat16)
    low = (exact - high.astype(jnp.float32)).astype(jnp.bfloat16)
    return jnp.concatenate([high, low], axis=1)


def with_ones(v):
    return jnp.concatenate([v, jnp.ones_like(v)], axis=1)


def across(column, width):
    return jnp.tile(column, (1, width // column.shape[1]))


def by_sublane(a):
    out = a[:8]
    for r in range(8, a.shape[0], 8):
        out = jnp.maximum(out, a[r : r + 8])
    return out


def own_kernel(heads, q_ref, kv_ref, m_ref, l_ref, a_ref, hm_ref):
    rows = q_ref.shape[0]
    k = kv_ref[:, :HEAD_SIZE]
    kk = jnp.concatenate([k, k], axis=1)
    ve = with_ones(kv_ref[:, HEAD_SIZE:])
    seen = lax.broadcasted_iota(jnp.int32, (rows, rows), 0) >= lax.broadcasted_iota(
        jnp.int32, (rows, rows), 1
    )
    for h in range(heads):
        q = scaled_queries(q_ref[:, h * HEAD_SIZE : (h + 1) * HEAD_SIZE])
        s = jnp.where(seen, dot_nt(q, kk), LOW)
        m = jnp.broadcast_to(jnp.max(s, axis=1, keepdims=True), (rows, HEAD_SIZE))
        p = jnp.exp2(s - across(m, rows)).astype(jnp.bfloat16)
        o = jnp.dot(p, ve, preferred_element_type=jnp.float32)
        m_ref[h] = m
        a_ref[h] = o[:, :HEAD_SIZE]
        l_ref[h] = o[:, HEAD_SIZE:]
        hm_ref[h] = by_sublane(m)


def more_kernel(heads, sources, counts, last, at_ref, q_ref, own_ref, *refs):
    n = len(counts)
    pieces, refs = refs[:n], refs[n:]
    if last:
        (m_in, l_in, a_in, hm_in, out_ref, hm_out, kk, ve) = refs
    else:
        (m_in, l_in, a_in, hm_in, m_ref, l_ref, a_ref, hm_out, kk, ve) = refs
    rows = q_ref.shape[0]
    total = sum(counts)
    place = at_ref[0]
    z, x = place // X, place % X
    base, visible = 0, []
    for ref, count, source in zip(pieces, counts, sources):
        size = count // len(source)
        for i, (dz, fixed_z, dx, zs) in enumerate(source):
            from_z = lax.rem(z + zs - dz, zs) if fixed_z is None else fixed_z
            came_from = from_z * X + lax.rem(x + X - dx, X)
            visible.append((ref, i * size, base, size, came_from < place))
            base += size
    some = visible[0][-1]
    for piece in visible[1:]:
        some = jnp.logical_or(some, piece[-1])

    tiles, at = [], 0
    while at < total:
        size = min(1024, total - at)
        tiles.append((at, size))
        at += size

    def columns(h):
        if isinstance(h, int):
            return pl.ds(h * HEAD_SIZE, HEAD_SIZE)
        return pl.ds(pl.multiple_of(h * HEAD_SIZE, HEAD_SIZE), HEAD_SIZE)

    def put(h, m, l, a, top):
        if last:
            out_ref[:, columns(h)] = (a / l).astype(out_ref.dtype)
        else:
            l_ref[h] = l
            a_ref[h] = a
            m_ref[h] = m
        top = jnp.maximum(hm_in[h], top)
        if last:
            peak = jnp.max(jnp.max(top, axis=0, keepdims=True), axis=1, keepdims=True)
            lane = lax.broadcasted_iota(jnp.int32, hm_out.shape, 1)
            hm_out[...] = jnp.where(lane == h, peak * (1.0 / LOG2E), hm_out[...])
        else:
            hm_out[h] = top

    def per_head(body, first):
        if heads <= HEADS_AT_ONCE:
            for h in range(heads):
                first = body(h, first)
            return first

        def some_heads(i, carry):
            for j in range(HEADS_AT_ONCE):
                carry = body(i * HEADS_AT_ONCE + j, carry)
            return carry

        return lax.fori_loop(0, heads // HEADS_AT_ONCE, some_heads, first)

    @pl.when(jnp.logical_not(some))
    def _():
        def unchanged(h, carry):
            put(h, m_in[h], l_in[h], a_in[h], hm_in[h])
            return carry

        lax.fori_loop(0, heads, unchanged, 0)

    @pl.when(some)
    def _():
        first_key = own_ref[0:1, :HEAD_SIZE]
        for ref, start, base, size, earlier in visible:
            k = jnp.where(
                earlier,
                ref[start : start + size, :HEAD_SIZE],
                jnp.broadcast_to(first_key, (size, HEAD_SIZE)),
            )
            v = ref[start : start + size, HEAD_SIZE:]
            at = pl.ds(base, size)
            kk[at, :HEAD_SIZE] = k
            kk[at, HEAD_SIZE:] = k
            ve[at, :HEAD_SIZE] = jnp.where(earlier, v, jnp.zeros_like(v))
            ve[at, HEAD_SIZE:] = jnp.where(earlier, jnp.ones_like(v), jnp.zeros_like(v))

        def head(h, largest):
            q = scaled_queries(q_ref[:, columns(h)])
            m = m_in[h]
            step = jnp.full((rows, HEAD_SIZE), LOW, jnp.float32)
            o = None
            for start, size in tiles:
                d = dot_nt(q, kk[start : start + size]) - across(m, size)
                for j in range(0, size, HEAD_SIZE):
                    step = jnp.maximum(step, d[:, j : j + HEAD_SIZE])
                p = jnp.exp2(d).astype(jnp.bfloat16)
                pv = jnp.dot(p, ve[start : start + size], preferred_element_type=jnp.float32)
                o = pv if o is None else o + pv
            put(h, m, l_in[h] + o[:, HEAD_SIZE:], a_in[h] + o[:, :HEAD_SIZE], by_sublane(step + m))
            return jnp.maximum(largest, by_sublane(step))

        largest = per_head(head, jnp.full((8, HEAD_SIZE), LOW, jnp.float32))

        @pl.when(jnp.max(largest) > LARGEST_STEP)
        def _():
            def again(h, carry):
                q = scaled_queries(q_ref[:, columns(h)])

                def tile(i, state):
                    m, l, a = state
                    at = pl.ds(pl.multiple_of(i * HEAD_SIZE, HEAD_SIZE), HEAD_SIZE)
                    s = dot_nt(q, kk[at])
                    new = jnp.maximum(m, jnp.broadcast_to(jnp.max(s, axis=1, keepdims=True), m.shape))
                    p = jnp.exp2(s - new).astype(jnp.bfloat16)
                    o = jnp.dot(p, ve[at], preferred_element_type=jnp.float32)
                    keep = jnp.exp2(m - new)
                    return new, l * keep + o[:, HEAD_SIZE:], a * keep + o[:, :HEAD_SIZE]

                m, l, a = lax.fori_loop(0, total // HEAD_SIZE, tile, (m_in[h], l_in[h], a_in[h]))
                put(h, m, l, a, by_sublane(m))
                return carry

            lax.fori_loop(0, heads, again, 0)


VMEM = pl.BlockSpec(memory_space=pltpu.VMEM)
SMEM = pl.BlockSpec(memory_space=pltpu.SMEM)


def state_types(heads, rows):
    wide = jax.ShapeDtypeStruct((heads, rows, HEAD_SIZE), jnp.float32)
    return [wide, wide, wide, jax.ShapeDtypeStruct((heads, 8, HEAD_SIZE), jnp.float32)]


def cost(rows, heads, keys):
    return pl.CostEstimate(
        flops=4 * rows * heads * keys * HEAD_SIZE,
        bytes_accessed=2 * rows * heads * HEAD_SIZE,
        transcendentals=rows * heads * keys,
    )


def attend_own(q, kv, heads):
    rows = q.shape[0]
    return pl.pallas_call(
        lambda *refs: own_kernel(heads, *refs),
        out_shape=state_types(heads, rows),
        in_specs=[VMEM, VMEM],
        out_specs=[VMEM] * 4,
        compiler_params=pltpu.CompilerParams(vmem_limit_bytes=40 << 20),
        cost_estimate=cost(rows, heads, rows),
        name="attend_own",
    )(q, kv)


def attend_more(at, q, kv, pieces, sources, state, heads, name, last=False):
    rows = q.shape[0]
    counts = [p.shape[0] for p in pieces]
    total = sum(counts)
    types = state_types(heads, rows)
    scratch = [pltpu.VMEM((total, 2 * HEAD_SIZE), jnp.bfloat16)] * 2
    if last:
        out_shape = [
            jax.ShapeDtypeStruct(q.shape, jnp.bfloat16),
            jax.ShapeDtypeStruct((8, heads), jnp.float32),
        ]
    else:
        out_shape = types
    return pl.pallas_call(
        lambda *refs: more_kernel(heads, sources, counts, last, *refs),
        out_shape=out_shape,
        in_specs=[SMEM] + [VMEM] * (2 + len(pieces) + 4),
        out_specs=[VMEM] * len(out_shape),
        scratch_shapes=scratch,
        compiler_params=pltpu.CompilerParams(vmem_limit_bytes=40 << 20),
        cost_estimate=cost(rows, heads, total),
        name=name,
    )(at, q, kv, *pieces, *state)


def scale_kernel(tp_ref, everyones_ref, wq_ref, kw_ref, hm_ref, wq_out, kw_out):
    tp_size, heads = everyones_ref.shape[1:]
    maxima = jnp.max(everyones_ref[...], axis=0)
    mine = lax.broadcasted_iota(jnp.int32, maxima.shape, 0) == tp_ref[0]
    own = jnp.max(jnp.where(mine, maxima, LOW), axis=0, keepdims=True)
    hm_ref[...] = own
    clip = CLIP_THRESHOLD / jnp.maximum(jnp.max(maxima, axis=1, keepdims=True), CLIP_THRESHOLD)
    own_clip = CLIP_THRESHOLD / jnp.maximum(jnp.max(own, axis=1, keepdims=True), CLIP_THRESHOLD)
    factor = CLIP_THRESHOLD / jnp.maximum(own, CLIP_THRESHOLD) / jnp.sqrt(own_clip)
    root = jnp.sqrt(clip)
    for h in range(heads):
        at = pl.ds(h * HEAD_SIZE, HEAD_SIZE)
        wq_out[:, at] = (wq_ref[:, at].astype(jnp.float32) * factor[:, h : h + 1]).astype(wq_out.dtype)
    for g in range(tp_size):
        at = pl.ds(g * HEAD_SIZE, HEAD_SIZE)
        kw_out[:, at] = (kw_ref[:, at].astype(jnp.float32) * root[g : g + 1]).astype(kw_out.dtype)


def scale_weights(tp_at, everyones, w_query, key_weight):
    heads = everyones.shape[2]
    return pl.pallas_call(
        scale_kernel,
        out_shape=[
            jax.ShapeDtypeStruct((1, heads), jnp.float32),
            jax.ShapeDtypeStruct(w_query.shape, w_query.dtype),
            jax.ShapeDtypeStruct(key_weight.shape, key_weight.dtype),
        ],
        in_specs=[SMEM] + [VMEM] * 3,
        out_specs=[VMEM] * 3,
        compiler_params=pltpu.CompilerParams(vmem_limit_bytes=16 << 20),
        name="scale_weights",
    )(tp_at, everyones, w_query, key_weight)


def shards(queries, keys, values, w_query, key_weight):
    heads = queries.shape[1] // HEAD_SIZE
    seq_size, tp_size = lax.axis_size("seq"), lax.axis_size("tp")
    zs = seq_size // X
    place = lax.axis_index("seq")
    at = place.reshape(1).astype(jnp.int32)

    def moved(a, dz, dx):
        pairs = [
            (((z - dz) % zs) * X + (x - dx) % X, z * X + x) for z in range(zs) for x in range(X)
        ]
        return lax.ppermute(a, "seq", pairs)

    kv = jnp.concatenate([keys, values], axis=1)
    half_a, half_b = kv[:A_ROWS], kv[A_ROWS:]
    state = attend_own(queries, kv, heads)

    b_x = {dx: moved(half_b, 0, dx) for dx in (1, 3, 2)}
    columns = [[z * X + x for z in range(zs)] for x in range(X)]
    column = lax.all_to_all(
        jnp.broadcast_to(half_a[None], (zs, *half_a.shape)),
        "seq",
        0,
        0,
        axis_index_groups=columns,
        tiled=True,
    ).reshape(zs * A_ROWS, kv.shape[1])
    layer = jnp.concatenate([half_b, b_x[1], b_x[2], b_x[3]], axis=0)
    b_up, b_down = [layer], [layer]
    for k in range(1, zs // 2 + 1):
        b_up.append(moved(b_up[-1], 1, 0))
        if k < zs // 2:
            b_down.append(moved(b_down[-1], -1, 0))
    a_x = {dx: moved(column, 0, dx) for dx in (1, 3, 2)}

    def more(state, name, parts, last=False):
        pieces, sources = zip(*parts)
        return attend_more(at, queries, kv, pieces, sources, state, heads, name, last)

    def b_part(k):
        return (b_up[k] if k > 0 else b_down[-k], [(k % zs, None, dx, zs) for dx in range(X)])

    def a_part(held, dx):
        return (held, [(None, z, dx, zs) for z in range(zs)])

    state = more(
        state,
        "attend_1",
        [(b_x[dx], [(0, None, dx, zs)]) for dx in (1, 2, 3)] + [a_part(column, 0)],
    )
    state = more(state, "attend_2", [b_part(1), b_part(-1)])
    state = more(state, "attend_3", [b_part(2), b_part(-2)])
    state = more(state, "attend_4", [a_part(a_x[dx], dx) for dx in (1, 2, 3)])
    state = more(state, "attend_5", [b_part(3), b_part(-3)])
    attended, head_top = more(state, "attend_6", [b_part(4)], last=True)

    devices = seq_size * tp_size
    everyones = lax.all_to_all(
        jnp.broadcast_to(head_top[None, :1], (devices, 1, heads)),
        ("seq", "tp"),
        0,
        0,
        tiled=True,
    ).reshape(seq_size, tp_size, heads)
    tp_at = lax.axis_index("tp").reshape(1).astype(jnp.int32)
    head_max, w_query_clipped, clipped_key_weight = scale_weights(
        tp_at, everyones, w_query, key_weight
    )
    return (attended, head_max.reshape(heads), w_query_clipped, clipped_key_weight)


def solution(mesh):
    in_specs = (P("seq", "tp"), P("seq", "tp"), P("seq", "tp"), P("seq", "tp"), P("seq", None))
    out_specs = (P("seq", "tp"), P("tp"), P("seq", "tp"), P("seq", None))
    return jax.shard_map(shards, mesh=mesh, in_specs=in_specs, out_specs=out_specs, check_vma=False)
```

```python
import jax
import jax.numpy as jnp
from jax import lax
from jax.experimental import pallas as pl
from jax.experimental.pallas import tpu as pltpu
from jax.sharding import PartitionSpec as P


HEAD_SIZE = 128
CLIP_THRESHOLD = 10.0
LOG2E = 1.4426950408889634
SCALE = HEAD_SIZE**-0.5 * LOG2E
LARGEST_STEP = 100.0
LOW = -1e30
X = 4
A_ROWS = 128
VMEM_LIMIT = 20 << 20
TILE = 1024


NT = (((1,), (1,)), ((), ()))
VMEM = pl.BlockSpec(memory_space=pltpu.VMEM)
SMEM = pl.BlockSpec(memory_space=pltpu.SMEM)


def logits_of(q, k):
    return lax.dot_general(q, k, NT, preferred_element_type=jnp.float32) * SCALE


def weigh(p, ve):
    return jnp.dot(p.astype(jnp.bfloat16), ve, preferred_element_type=jnp.float32)


def with_ones(v):
    return jnp.concatenate([v, jnp.ones_like(v)], axis=1)


def across(column, width):
    return jnp.tile(column, (1, width // column.shape[1]))


def row_max(s):
    return jnp.broadcast_to(jnp.max(s, axis=1, keepdims=True), (s.shape[0], HEAD_SIZE))


def by_sublane(a):
    out = a[:8]
    for r in range(8, a.shape[0], 8):
        out = jnp.maximum(out, a[r : r + 8])
    return out


def columns(h):
    if isinstance(h, int):
        return pl.ds(h * HEAD_SIZE, HEAD_SIZE)
    return pl.ds(pl.multiple_of(h * HEAD_SIZE, HEAD_SIZE), HEAD_SIZE)


def pieces_of(at_ref, refs, sources):
    place = at_ref[0]
    z, x = place // X, place % X
    base, found = 0, []
    for ref, source in zip(refs, sources):
        size = ref.shape[0] // len(source)
        for i, (dz, fixed_z, dx, zs) in enumerate(source):
            from_z = lax.rem(z + zs - dz, zs) if fixed_z is None else fixed_z
            came_from = from_z * X + lax.rem(x + X - dx, X)
            found.append((ref, i * size, base, size, came_from < place))
            base += size
    return found


def gather(pieces, own_ref, k_all, ve):
    first_key = own_ref[0:1, :HEAD_SIZE]
    for ref, start, base, size, earlier in pieces:
        rows = pl.ds(start, size)
        at = pl.ds(base, size)
        k_all[at] = jnp.where(
            earlier, ref[rows, :HEAD_SIZE], jnp.broadcast_to(first_key, (size, HEAD_SIZE))
        )
        if ve is not None:
            v = ref[rows, HEAD_SIZE:]
            ve[at, :HEAD_SIZE] = jnp.where(earlier, v, jnp.zeros_like(v))
            ve[at, HEAD_SIZE:] = jnp.where(earlier, jnp.ones_like(v), jnp.zeros_like(v))


def lane_of(h, shape):
    return lax.broadcasted_iota(jnp.int32, shape, 1) == h


def spread(per_head, h):
    if isinstance(h, int):
        return jnp.broadcast_to(per_head[:, h : h + 1], per_head.shape)
    return row_max(jnp.where(lane_of(h, per_head.shape), per_head, LOW))


def attend_kernel(heads, at_once, sources, total, first, last, at_ref, q_ref, own_ref, *refs):
    n = len(sources)
    parts, refs = refs[:n], refs[n:]
    if not first:
        (m_in, l_in, a_in), refs = refs[:3], refs[3:]
        if not last:
            hm_in, refs = refs[0], refs[1:]
    if last:
        out_ref, k_all, ve = refs
    else:
        m_ref, l_ref, a_ref, hm_ref, k_all, ve = refs
    rows = q_ref.shape[0]
    pieces = pieces_of(at_ref, parts, sources)
    tiles = [(at, min(TILE, total - at)) for at in range(0, total, TILE)]
    per_head = (rows, HEAD_SIZE)
    none = jnp.zeros(per_head, jnp.float32)

    def before(h, q):
        if not first:
            top = None if last else hm_in[h]
            return spread(m_in[...], h), spread(l_in[...], h), a_in[h], top
        seen = lax.broadcasted_iota(jnp.int32, (rows, rows), 0) >= lax.broadcasted_iota(
            jnp.int32, (rows, rows), 1
        )
        s = jnp.where(seen, logits_of(q, own_ref[:, :HEAD_SIZE]), LOW)
        m = row_max(s)
        o = weigh(jnp.exp2(s - across(m, rows)), with_ones(own_ref[:, HEAD_SIZE:]))
        return m, o[:, HEAD_SIZE:], o[:, :HEAD_SIZE], by_sublane(m)

    def put(h, m, l, a, top, held):
        if last:
            out_ref[:, columns(h)] = (a / l).astype(out_ref.dtype)
            return held
        a_ref[h] = a
        hm_ref[h] = top
        here = lane_of(h, per_head)
        return jnp.where(here, m, held[0]), jnp.where(here, l, held[1])

    def keep(held):
        if not last:
            m_ref[...], l_ref[...] = held

    def fast():
        gather(pieces, own_ref, k_all, ve)
        largest = jnp.full((8, HEAD_SIZE), LOW, jnp.float32)

        def head(h, carry):
            largest, held = carry
            q = q_ref[:, columns(h)]
            m, l, a, top = before(h, q)
            step = jnp.full(per_head, LOW, jnp.float32)
            o = None
            for start, size in tiles:
                d = logits_of(q, k_all[start : start + size]) - across(m, size)
                for j in range(0, size, HEAD_SIZE):
                    step = jnp.maximum(step, d[:, j : j + HEAD_SIZE])
                pv = weigh(jnp.exp2(d), ve[start : start + size])
                o = pv if o is None else o + pv
            largest = jnp.maximum(largest, by_sublane(step))
            if not last:
                top = jnp.maximum(top, by_sublane(step + m))
            held = put(h, m, l + o[:, HEAD_SIZE:], a + o[:, :HEAD_SIZE], top, held)
            return largest, held

        carry = largest, (none, none)
        if at_once < heads:

            def some_heads(i, carry):
                for j in range(at_once):
                    carry = head(i * at_once + j, carry)
                return carry

            carry = lax.fori_loop(0, heads // at_once, some_heads, carry)
        else:
            for h in range(heads):
                carry = head(h, carry)
        largest, held = carry
        keep(held)

        @pl.when(jnp.max(largest) > LARGEST_STEP)
        def _():
            keep(lax.fori_loop(0, heads, again, (none, none)))

    def again(h, held):
        q = q_ref[:, columns(h)]
        m, l, a, top = before(h, q)

        def tile(i, state):
            m, l, a = state
            at = pl.ds(pl.multiple_of(i * HEAD_SIZE, HEAD_SIZE), HEAD_SIZE)
            s = logits_of(q, k_all[at])
            new = jnp.maximum(m, row_max(s))
            o = weigh(jnp.exp2(s - new), ve[at])
            kept = jnp.exp2(m - new)
            return new, l * kept + o[:, HEAD_SIZE:], a * kept + o[:, :HEAD_SIZE]

        m, l, a = lax.fori_loop(0, total // HEAD_SIZE, tile, (m, l, a))
        return put(h, m, l, a, None if last else jnp.maximum(top, by_sublane(m)), held)

    if first:
        fast()
        return
    some = pieces[0][-1]
    for piece in pieces[1:]:
        some = jnp.logical_or(some, piece[-1])

    @pl.when(jnp.logical_not(some))
    def _():
        def unchanged(h, held):
            return put(h, none, spread(l_in[...], h), a_in[h], None if last else hm_in[h], held)

        lax.fori_loop(0, heads, unchanged, (none, none))
        if not last:
            keep((m_in[...], l_in[...]))

    pl.when(some)(fast)


def top_kernel(heads, sources, total, at_ref, q_ref, own_ref, *refs):
    n = len(sources)
    parts, (hm_in, out_ref, k_all) = refs[:n], refs[n:]
    gather(pieces_of(at_ref, parts, sources), own_ref, k_all, None)
    lane = lax.broadcasted_iota(jnp.int32, (8, heads), 1)
    tops = jnp.full((8, heads), LOW, jnp.float32)
    for h in range(heads):
        s = logits_of(q_ref[:, columns(h)], k_all[...])
        best = s[:, :HEAD_SIZE]
        for j in range(HEAD_SIZE, total, HEAD_SIZE):
            best = jnp.maximum(best, s[:, j : j + HEAD_SIZE])
        best = jnp.maximum(hm_in[h], by_sublane(best))
        peak = jnp.max(jnp.max(best, axis=0, keepdims=True), axis=1, keepdims=True)
        tops = jnp.where(lane == h, peak * (1.0 / LOG2E), tops)
    out_ref[...] = tops


def cost(rows, heads, keys):
    return pl.CostEstimate(
        flops=4 * rows * heads * keys * HEAD_SIZE,
        bytes_accessed=2 * rows * heads * HEAD_SIZE,
        transcendentals=rows * heads * keys,
    )


def attend(at, q, kv, parts, sources, state, heads, at_once, last=False):
    rows = q.shape[0]
    total = sum(p.shape[0] for p in parts)
    first = state is None
    if last:
        out_shape = [jax.ShapeDtypeStruct(q.shape, jnp.bfloat16)]
    else:
        wide = jax.ShapeDtypeStruct((heads, rows, HEAD_SIZE), jnp.float32)
        thin = jax.ShapeDtypeStruct((rows, HEAD_SIZE), jnp.float32)
        out_shape = [thin, thin, wide] + [jax.ShapeDtypeStruct((heads, 8, HEAD_SIZE), jnp.float32)]
    held = [] if first else list(state[:3] if last else state)
    return pl.pallas_call(
        lambda *refs: attend_kernel(heads, at_once, sources, total, first, last, *refs),
        out_shape=out_shape,
        in_specs=[SMEM] + [VMEM] * (2 + len(parts) + len(held)),
        out_specs=[VMEM] * len(out_shape),
        scratch_shapes=[
            pltpu.VMEM((total, HEAD_SIZE), jnp.bfloat16),
            pltpu.VMEM((total, 2 * HEAD_SIZE), jnp.bfloat16),
        ],
        compiler_params=pltpu.CompilerParams(vmem_limit_bytes=VMEM_LIMIT),
        cost_estimate=cost(rows, heads, total + rows * first),
    )(at, q, kv, *parts, *held)


def local_tops(at, q, kv, parts, sources, hm, heads):
    total = sum(p.shape[0] for p in parts)
    return pl.pallas_call(
        lambda *refs: top_kernel(heads, sources, total, *refs),
        out_shape=jax.ShapeDtypeStruct((8, heads), jnp.float32),
        in_specs=[SMEM] + [VMEM] * (3 + len(parts)),
        out_specs=VMEM,
        scratch_shapes=[pltpu.VMEM((total, HEAD_SIZE), jnp.bfloat16)],
        compiler_params=pltpu.CompilerParams(vmem_limit_bytes=VMEM_LIMIT),
        cost_estimate=cost(q.shape[0], heads, total // 2),
    )(at, q, kv, *parts, hm)


def pack_kernel(k_ref, v_ref, kv_ref, b_ref, a_ref):
    both = jnp.concatenate([k_ref[...], v_ref[...]], axis=1)
    kv_ref[...] = both
    b_ref[...] = both[A_ROWS:]
    for i in range(a_ref.shape[0]):
        a_ref[i] = both[:A_ROWS]


def pack(keys, values, copies):
    rows, wide = keys.shape[0], 2 * keys.shape[1]

    def of(*shape):
        return jax.ShapeDtypeStruct(shape, keys.dtype)

    return pl.pallas_call(
        pack_kernel,
        out_shape=[of(rows, wide), of(rows - A_ROWS, wide), of(copies, A_ROWS, wide)],
        in_specs=[VMEM] * 2,
        out_specs=[VMEM] * 3,
        compiler_params=pltpu.CompilerParams(vmem_limit_bytes=VMEM_LIMIT),
        name="pack",
    )(keys, values)


def scale_kernel(tp_ref, everyones_ref, wq_ref, kw_ref, hm_ref, wq_out, kw_out):
    tp_size, heads = everyones_ref.shape[1:]
    maxima = jnp.max(everyones_ref[...], axis=0)
    mine = lax.broadcasted_iota(jnp.int32, maxima.shape, 0) == tp_ref[0]
    own = jnp.max(jnp.where(mine, maxima, LOW), axis=0, keepdims=True)
    hm_ref[...] = own
    clip = CLIP_THRESHOLD / jnp.maximum(jnp.max(maxima, axis=1, keepdims=True), CLIP_THRESHOLD)
    own_clip = CLIP_THRESHOLD / jnp.maximum(jnp.max(own, axis=1, keepdims=True), CLIP_THRESHOLD)
    factor = CLIP_THRESHOLD / jnp.maximum(own, CLIP_THRESHOLD) / jnp.sqrt(own_clip)
    root = jnp.sqrt(clip)
    for h in range(heads):
        at = columns(h)
        wq_out[:, at] = (wq_ref[:, at].astype(jnp.float32) * factor[:, h : h + 1]).astype(wq_out.dtype)
    for g in range(tp_size):
        at = columns(g)
        kw_out[:, at] = (kw_ref[:, at].astype(jnp.float32) * root[g : g + 1]).astype(kw_out.dtype)


def scale_weights(tp_at, everyones, w_query, key_weight):
    heads = everyones.shape[2]
    return pl.pallas_call(
        scale_kernel,
        out_shape=[
            jax.ShapeDtypeStruct((1, heads), jnp.float32),
            jax.ShapeDtypeStruct(w_query.shape, w_query.dtype),
            jax.ShapeDtypeStruct(key_weight.shape, key_weight.dtype),
        ],
        in_specs=[SMEM] + [VMEM] * 3,
        out_specs=[VMEM] * 3,
        compiler_params=pltpu.CompilerParams(vmem_limit_bytes=VMEM_LIMIT),
        name="scale_weights",
    )(tp_at, everyones, w_query, key_weight)


def shards(queries, keys, values, w_query, key_weight):
    heads = queries.shape[1] // HEAD_SIZE
    seq_size, tp_size = lax.axis_size("seq"), lax.axis_size("tp")
    zs = seq_size // X
    at = lax.axis_index("seq").reshape(1).astype(jnp.int32)

    def moved(a, dz, dx):
        pairs = [
            (((z - dz) % zs) * X + (x - dx) % X, z * X + x) for z in range(zs) for x in range(X)
        ]
        return lax.ppermute(a, "seq", pairs)

    kv, half_b, half_a = pack(keys, values, zs)

    b_x = {dx: moved(half_b, 0, dx) for dx in (1, 3, 2)}
    along_z = [[z * X + x for z in range(zs)] for x in range(X)]
    column = lax.all_to_all(half_a, "seq", 0, 0, axis_index_groups=along_z, tiled=True)
    column = column.reshape(zs * A_ROWS, kv.shape[1])
    layer = jnp.concatenate([half_b, b_x[1], b_x[2], b_x[3]], axis=0)
    b_up, b_down = [layer], [layer]
    for k in range(1, zs // 2 + 1):
        b_up.append(moved(b_up[-1], 1, 0))
        if k < zs // 2:
            b_down.append(moved(b_down[-1], -1, 0))
    a_x = {dx: moved(column, 0, dx) for dx in (1, 3, 2)}

    def b_part(k):
        return (b_up[k] if k > 0 else b_down[-k], [(k % zs, None, dx, zs) for dx in range(X)])

    def a_part(held, dx):
        return (held, [(None, z, dx, zs) for z in range(zs)])

    def more(state, parts, last=False, at_once=heads):
        parts, sources = zip(*parts)
        return attend(at, queries, kv, parts, sources, state, heads, at_once, last)

    near = [(b_x[dx], [(0, None, dx, zs)]) for dx in (1, 2, 3)] + [a_part(column, 0)]
    state = more(None, near)
    state = more(state, [b_part(1), b_part(-1)])
    state = more(state, [b_part(2), b_part(-2)])
    state = more(state, [a_part(a_x[1], 1)], at_once=heads // 2)
    state = more(state, [a_part(a_x[3], 3)])
    state = more(state, [a_part(a_x[2], 2), b_part(3), b_part(-3)])
    final_part, final_source = b_part(4)
    tops = local_tops(at, queries, kv, [final_part], [final_source], state[3], heads)
    (attended,) = more(state, [b_part(4)], last=True, at_once=1)

    devices = seq_size * tp_size
    everyones = lax.all_to_all(
        jnp.broadcast_to(tops[None, :1], (devices, 1, heads)), ("seq", "tp"), 0, 0, tiled=True
    ).reshape(seq_size, tp_size, heads)
    tp_at = lax.axis_index("tp").reshape(1).astype(jnp.int32)
    head_max, w_query_clipped, clipped_key_weight = scale_weights(
        tp_at, everyones, w_query, key_weight
    )
    return (attended, head_max.reshape(heads), w_query_clipped, clipped_key_weight)


def solution(mesh):
    in_specs = (P("seq", "tp"), P("seq", "tp"), P("seq", "tp"), P("seq", "tp"), P("seq", None))
    out_specs = (P("seq", "tp"), P("tp"), P("seq", "tp"), P("seq", None))

    return jax.shard_map(shards, mesh=mesh, in_specs=in_specs, out_specs=out_specs, check_vma=False)
```

```python
import jax
import jax.numpy as jnp
from jax import lax
from jax.experimental import pallas as pl
from jax.experimental.pallas import tpu as pltpu
from jax.sharding import PartitionSpec as P


HEAD_SIZE = 128
CLIP_THRESHOLD = 10.0
LOG2E = 1.4426950408889634
SCALE = HEAD_SIZE**-0.5 * LOG2E
LARGEST_STEP = 100.0
LOW = -1e30
X = 4
A_ROWS = 128
VMEM_LIMIT = 20 << 20
TILE = 1024


NT = (((1,), (1,)), ((), ()))
VMEM = pl.BlockSpec(memory_space=pltpu.VMEM)


def logits_of(q, k):
    return lax.dot_general(q, k, NT, preferred_element_type=jnp.float32) * SCALE


def weigh(p, ve):
    return jnp.dot(p.astype(jnp.bfloat16), ve, preferred_element_type=jnp.float32)


def with_ones(v):
    return jnp.concatenate([v, jnp.ones_like(v)], axis=1)


def across(column, width):
    return jnp.tile(column, (1, width // column.shape[1]))


def row_max(s):
    return jnp.broadcast_to(jnp.max(s, axis=1, keepdims=True), (s.shape[0], HEAD_SIZE))


def by_sublane(a):
    out = a[:8]
    for r in range(8, a.shape[0], 8):
        out = jnp.maximum(out, a[r : r + 8])
    return out


def columns(h):
    if isinstance(h, int):
        return pl.ds(h * HEAD_SIZE, HEAD_SIZE)
    return pl.ds(pl.multiple_of(h * HEAD_SIZE, HEAD_SIZE), HEAD_SIZE)


def pieces_of(refs, sources):
    place = lax.axis_index("seq")
    z, x = place // X, place % X
    base, found = 0, []
    for ref, source in zip(refs, sources):
        size = ref.shape[0] // len(source)
        for i, (dz, fixed_z, dx, zs) in enumerate(source):
            from_z = lax.rem(z + zs - dz, zs) if fixed_z is None else fixed_z
            came_from = from_z * X + lax.rem(x + X - dx, X)
            found.append((ref, i * size, base, size, came_from < place))
            base += size
    return found


def gather(pieces, own_ref, k_all, ve):
    first_key = own_ref[0:1, :HEAD_SIZE]
    for ref, start, base, size, earlier in pieces:
        rows = pl.ds(start, size)
        at = pl.ds(base, size)
        k_all[at] = jnp.where(
            earlier, ref[rows, :HEAD_SIZE], jnp.broadcast_to(first_key, (size, HEAD_SIZE))
        )
        if ve is not None:
            v = ref[rows, HEAD_SIZE:]
            ve[at, :HEAD_SIZE] = jnp.where(earlier, v, jnp.zeros_like(v))
            ve[at, HEAD_SIZE:] = jnp.where(earlier, jnp.ones_like(v), jnp.zeros_like(v))


def lane_of(h, shape):
    return lax.broadcasted_iota(jnp.int32, shape, 1) == h


def spread(per_head, h):
    if isinstance(h, int):
        return jnp.broadcast_to(per_head[:, h : h + 1], per_head.shape)
    return row_max(jnp.where(lane_of(h, per_head.shape), per_head, LOW))


def attend_kernel(heads, at_once, sources, total, first, last, q_ref, own_ref, *refs):
    n = len(sources)
    parts, refs = refs[:n], refs[n:]
    if not first:
        (m_in, l_in, a_in), refs = refs[:3], refs[3:]
        if not last:
            hm_in, refs = refs[0], refs[1:]
    if last:
        out_ref, k_all, ve = refs
    else:
        m_ref, l_ref, a_ref, hm_ref, k_all, ve = refs
    rows = q_ref.shape[0]
    pieces = pieces_of(parts, sources)
    tiles = [(at, min(TILE, total - at)) for at in range(0, total, TILE)]
    per_head = (rows, HEAD_SIZE)
    none = jnp.zeros(per_head, jnp.float32)

    def before(h, q):
        if not first:
            top = None if last else hm_in[h]
            return spread(m_in[...], h), spread(l_in[...], h), a_in[h], top
        seen = lax.broadcasted_iota(jnp.int32, (rows, rows), 0) >= lax.broadcasted_iota(
            jnp.int32, (rows, rows), 1
        )
        s = jnp.where(seen, logits_of(q, own_ref[:, :HEAD_SIZE]), LOW)
        m = row_max(s)
        o = weigh(jnp.exp2(s - across(m, rows)), with_ones(own_ref[:, HEAD_SIZE:]))
        return m, o[:, HEAD_SIZE:], o[:, :HEAD_SIZE], by_sublane(m)

    def put(h, m, l, a, top, held):
        if last:
            out_ref[:, columns(h)] = (a / l).astype(out_ref.dtype)
            return held
        a_ref[h] = a
        hm_ref[h] = top
        here = lane_of(h, per_head)
        return jnp.where(here, m, held[0]), jnp.where(here, l, held[1])

    def keep(held):
        if not last:
            m_ref[...], l_ref[...] = held

    def fast():
        gather(pieces, own_ref, k_all, ve)
        largest = jnp.full((8, HEAD_SIZE), LOW, jnp.float32)

        def head(h, carry):
            largest, held = carry
            q = q_ref[:, columns(h)]
            m, l, a, top = before(h, q)
            step = jnp.full(per_head, LOW, jnp.float32)
            o = None
            for start, size in tiles:
                d = logits_of(q, k_all[start : start + size]) - across(m, size)
                for j in range(0, size, HEAD_SIZE):
                    step = jnp.maximum(step, d[:, j : j + HEAD_SIZE])
                pv = weigh(jnp.exp2(d), ve[start : start + size])
                o = pv if o is None else o + pv
            largest = jnp.maximum(largest, by_sublane(step))
            if not last:
                top = jnp.maximum(top, by_sublane(step + m))
            held = put(h, m, l + o[:, HEAD_SIZE:], a + o[:, :HEAD_SIZE], top, held)
            return largest, held

        carry = largest, (none, none)
        if at_once < heads:

            def some_heads(i, carry):
                for j in range(at_once):
                    carry = head(i * at_once + j, carry)
                return carry

            carry = lax.fori_loop(0, heads // at_once, some_heads, carry)
        else:
            for h in range(heads):
                carry = head(h, carry)
        largest, held = carry
        keep(held)

        @pl.when(jnp.max(largest) > LARGEST_STEP)
        def _():
            keep(lax.fori_loop(0, heads, again, (none, none)))

    def again(h, held):
        q = q_ref[:, columns(h)]
        m, l, a, top = before(h, q)

        def tile(i, state):
            m, l, a = state
            at = pl.ds(pl.multiple_of(i * HEAD_SIZE, HEAD_SIZE), HEAD_SIZE)
            s = logits_of(q, k_all[at])
            new = jnp.maximum(m, row_max(s))
            o = weigh(jnp.exp2(s - new), ve[at])
            kept = jnp.exp2(m - new)
            return new, l * kept + o[:, HEAD_SIZE:], a * kept + o[:, :HEAD_SIZE]

        m, l, a = lax.fori_loop(0, total // HEAD_SIZE, tile, (m, l, a))
        return put(h, m, l, a, None if last else jnp.maximum(top, by_sublane(m)), held)

    if first:
        fast()
        return
    some = pieces[0][-1]
    for piece in pieces[1:]:
        some = jnp.logical_or(some, piece[-1])

    @pl.when(jnp.logical_not(some))
    def _():
        def unchanged(h, held):
            return put(h, none, spread(l_in[...], h), a_in[h], None if last else hm_in[h], held)

        lax.fori_loop(0, heads, unchanged, (none, none))
        if not last:
            keep((m_in[...], l_in[...]))

    pl.when(some)(fast)


def top_kernel(heads, sources, total, q_ref, own_ref, *refs):
    n = len(sources)
    parts, (hm_in, out_ref, k_all) = refs[:n], refs[n:]
    gather(pieces_of(parts, sources), own_ref, k_all, None)
    lane = lax.broadcasted_iota(jnp.int32, (8, heads), 1)
    tops = jnp.full((8, heads), LOW, jnp.float32)
    for h in range(heads):
        s = logits_of(q_ref[:, columns(h)], k_all[...])
        best = s[:, :HEAD_SIZE]
        for j in range(HEAD_SIZE, total, HEAD_SIZE):
            best = jnp.maximum(best, s[:, j : j + HEAD_SIZE])
        best = jnp.maximum(hm_in[h], by_sublane(best))
        peak = jnp.max(jnp.max(best, axis=0, keepdims=True), axis=1, keepdims=True)
        tops = jnp.where(lane == h, peak * (1.0 / LOG2E), tops)
    out_ref[...] = tops


def cost(rows, heads, keys):
    return pl.CostEstimate(
        flops=4 * rows * heads * keys * HEAD_SIZE,
        bytes_accessed=2 * rows * heads * HEAD_SIZE,
        transcendentals=rows * heads * keys,
    )


def attend(q, kv, parts, sources, state, heads, at_once, last=False):
    rows = q.shape[0]
    total = sum(p.shape[0] for p in parts)
    first = state is None
    if last:
        out_shape = [jax.ShapeDtypeStruct(q.shape, jnp.bfloat16)]
    else:
        wide = jax.ShapeDtypeStruct((heads, rows, HEAD_SIZE), jnp.float32)
        thin = jax.ShapeDtypeStruct((rows, HEAD_SIZE), jnp.float32)
        out_shape = [thin, thin, wide] + [jax.ShapeDtypeStruct((heads, 8, HEAD_SIZE), jnp.float32)]
    held = [] if first else list(state[:3] if last else state)
    return pl.pallas_call(
        lambda *refs: attend_kernel(heads, at_once, sources, total, first, last, *refs),
        out_shape=out_shape,
        in_specs=[VMEM] * (2 + len(parts) + len(held)),
        out_specs=[VMEM] * len(out_shape),
        scratch_shapes=[
            pltpu.VMEM((total, HEAD_SIZE), jnp.bfloat16),
            pltpu.VMEM((total, 2 * HEAD_SIZE), jnp.bfloat16),
        ],
        compiler_params=pltpu.CompilerParams(vmem_limit_bytes=VMEM_LIMIT),
        cost_estimate=cost(rows, heads, total + rows * first),
    )(q, kv, *parts, *held)


def local_tops(q, kv, parts, sources, hm, heads):
    total = sum(p.shape[0] for p in parts)
    return pl.pallas_call(
        lambda *refs: top_kernel(heads, sources, total, *refs),
        out_shape=jax.ShapeDtypeStruct((8, heads), jnp.float32),
        in_specs=[VMEM] * (3 + len(parts)),
        out_specs=VMEM,
        scratch_shapes=[pltpu.VMEM((total, HEAD_SIZE), jnp.bfloat16)],
        compiler_params=pltpu.CompilerParams(vmem_limit_bytes=VMEM_LIMIT),
        cost_estimate=cost(q.shape[0], heads, total // 2),
    )(q, kv, *parts, hm)


def scale_kernel(everyones_ref, wq_ref, kw_ref, hm_ref, wq_out, kw_out):
    tp_size, heads = everyones_ref.shape[1:]
    maxima = jnp.max(everyones_ref[...], axis=0)
    mine = lax.broadcasted_iota(jnp.int32, maxima.shape, 0) == lax.axis_index("tp")
    own = jnp.max(jnp.where(mine, maxima, LOW), axis=0, keepdims=True)
    hm_ref[...] = own
    clip = CLIP_THRESHOLD / jnp.maximum(jnp.max(maxima, axis=1, keepdims=True), CLIP_THRESHOLD)
    own_clip = CLIP_THRESHOLD / jnp.maximum(jnp.max(own, axis=1, keepdims=True), CLIP_THRESHOLD)
    factor = CLIP_THRESHOLD / jnp.maximum(own, CLIP_THRESHOLD) / jnp.sqrt(own_clip)
    root = jnp.sqrt(clip)
    for h in range(heads):
        at = columns(h)
        wq_out[:, at] = (wq_ref[:, at].astype(jnp.float32) * factor[:, h : h + 1]).astype(wq_out.dtype)
    for g in range(tp_size):
        at = columns(g)
        kw_out[:, at] = (kw_ref[:, at].astype(jnp.float32) * root[g : g + 1]).astype(kw_out.dtype)


def scale_weights(everyones, w_query, key_weight):
    heads = everyones.shape[2]
    return pl.pallas_call(
        scale_kernel,
        out_shape=[
            jax.ShapeDtypeStruct((1, heads), jnp.float32),
            jax.ShapeDtypeStruct(w_query.shape, w_query.dtype),
            jax.ShapeDtypeStruct(key_weight.shape, key_weight.dtype),
        ],
        in_specs=[VMEM] * 3,
        out_specs=[VMEM] * 3,
        compiler_params=pltpu.CompilerParams(vmem_limit_bytes=VMEM_LIMIT),
        name="scale_weights",
    )(everyones, w_query, key_weight)


def shards(queries, keys, values, w_query, key_weight):
    heads = queries.shape[1] // HEAD_SIZE
    seq_size, tp_size = lax.axis_size("seq"), lax.axis_size("tp")
    zs = seq_size // X

    def moved(a, dz, dx):
        pairs = [
            (((z - dz) % zs) * X + (x - dx) % X, z * X + x) for z in range(zs) for x in range(X)
        ]
        return lax.ppermute(a, "seq", pairs)

    kv = jnp.concatenate([keys, values], axis=1)
    half_a, half_b = kv[:A_ROWS], kv[A_ROWS:]

    b_x = {dx: moved(half_b, 0, dx) for dx in (1, 3, 2)}
    along_z = [[z * X + x for z in range(zs)] for x in range(X)]
    column = lax.all_to_all(
        jnp.broadcast_to(half_a[None], (zs, *half_a.shape)),
        "seq",
        0,
        0,
        axis_index_groups=along_z,
        tiled=True,
    )
    column = column.reshape(zs * A_ROWS, kv.shape[1])
    layer = jnp.concatenate([half_b, b_x[1], b_x[2], b_x[3]], axis=0)
    b_up, b_down = [layer], [layer]
    for k in range(1, zs // 2 + 1):
        b_up.append(moved(b_up[-1], 1, 0))
        if k < zs // 2:
            b_down.append(moved(b_down[-1], -1, 0))
    a_x = {dx: moved(column, 0, dx) for dx in (1, 3, 2)}

    def b_part(k):
        return (b_up[k] if k > 0 else b_down[-k], [(k % zs, None, dx, zs) for dx in range(X)])

    def a_part(held, dx):
        return (held, [(None, z, dx, zs) for z in range(zs)])

    def more(state, parts, last=False, at_once=heads):
        parts, sources = zip(*parts)
        return attend(queries, kv, parts, sources, state, heads, at_once, last)

    near = [(b_x[dx], [(0, None, dx, zs)]) for dx in (1, 2, 3)] + [a_part(column, 0)]
    state = more(None, near)
    state = more(state, [b_part(1), b_part(-1)])
    state = more(state, [b_part(2), b_part(-2)])
    state = more(state, [a_part(a_x[1], 1)], at_once=heads // 2)
    state = more(state, [a_part(a_x[3], 3)])
    state = more(state, [a_part(a_x[2], 2), b_part(3), b_part(-3)])
    final_part, final_source = b_part(4)
    tops = local_tops(queries, kv, [final_part], [final_source], state[3], heads)
    (attended,) = more(state, [b_part(4)], last=True, at_once=1)

    devices = seq_size * tp_size
    everyones = lax.all_to_all(
        jnp.broadcast_to(tops[None, :1], (devices, 1, heads)), ("seq", "tp"), 0, 0, tiled=True
    ).reshape(seq_size, tp_size, heads)
    head_max, w_query_clipped, clipped_key_weight = scale_weights(everyones, w_query, key_weight)
    return (attended, head_max.reshape(heads), w_query_clipped, clipped_key_weight)


def solution(mesh):
    in_specs = (P("seq", "tp"), P("seq", "tp"), P("seq", "tp"), P("seq", "tp"), P("seq", None))
    out_specs = (P("seq", "tp"), P("tp"), P("seq", "tp"), P("seq", None))

    return jax.shard_map(shards, mesh=mesh, in_specs=in_specs, out_specs=out_specs, check_vma=False)
```

```python
import jax
import jax.numpy as jnp
from jax import lax
from jax.experimental import pallas as pl
from jax.experimental.pallas import tpu as pltpu
from jax.sharding import PartitionSpec as P


HEAD_SIZE = 128
CLIP_THRESHOLD = 10.0
LOG2E = 1.4426950408889634
SCALE = HEAD_SIZE**-0.5 * LOG2E
LARGEST_STEP = 100.0
LOW = -1e30
X = 4
A_ROWS = 144
VMEM_LIMIT = 20 << 20
TILE = 1280


NT = (((1,), (1,)), ((), ()))
VMEM = pl.BlockSpec(memory_space=pltpu.VMEM)


def logits_of(q, k):
    return lax.dot_general(q, k, NT, preferred_element_type=jnp.float32) * SCALE


def weigh(p, ve):
    return jnp.dot(p.astype(jnp.bfloat16), ve, preferred_element_type=jnp.float32)


def with_ones(v):
    return jnp.concatenate([v, jnp.ones_like(v)], axis=1)


def across(column, width):
    wide = jnp.tile(column, (1, -(-width // column.shape[1])))
    return wide[:, :width]


def row_max(s):
    return jnp.broadcast_to(jnp.max(s, axis=1, keepdims=True), (s.shape[0], HEAD_SIZE))


def by_sublane(a):
    out = a[:8]
    for r in range(8, a.shape[0], 8):
        out = jnp.maximum(out, a[r : r + 8])
    return out


def columns(h):
    if isinstance(h, int):
        return pl.ds(h * HEAD_SIZE, HEAD_SIZE)
    return pl.ds(pl.multiple_of(h * HEAD_SIZE, HEAD_SIZE), HEAD_SIZE)


def pieces_of(refs, sources):
    place = lax.axis_index("seq")
    z, x = place // X, place % X
    base, found = 0, []
    for ref, source in zip(refs, sources):
        size = ref.shape[0] // len(source)
        for i, (dz, fixed_z, dx, zs) in enumerate(source):
            from_z = lax.rem(z + zs - dz, zs) if fixed_z is None else fixed_z
            came_from = from_z * X + lax.rem(x + X - dx, X)
            found.append((ref, i * size, base, size, came_from < place))
            base += size
    return found


def gather(pieces, own_ref, k_all, ve):
    first_key = own_ref[0:1, :HEAD_SIZE]
    for ref, start, base, size, earlier in pieces:
        rows = pl.ds(start, size)
        at = pl.ds(base, size)
        k_all[at] = jnp.where(
            earlier, ref[rows, :HEAD_SIZE], jnp.broadcast_to(first_key, (size, HEAD_SIZE))
        )
        if ve is not None:
            v = ref[rows, HEAD_SIZE:]
            ve[at, :HEAD_SIZE] = jnp.where(earlier, v, jnp.zeros_like(v))
            ve[at, HEAD_SIZE:] = jnp.where(earlier, jnp.ones_like(v), jnp.zeros_like(v))


def lane_of(h, shape):
    return lax.broadcasted_iota(jnp.int32, shape, 1) == h


def spread(per_head, h):
    if isinstance(h, int):
        return jnp.broadcast_to(per_head[:, h : h + 1], per_head.shape)
    return row_max(jnp.where(lane_of(h, per_head.shape), per_head, LOW))


def attend_kernel(heads, at_once, sources, total, first, last, q_ref, own_ref, *refs):
    n = len(sources)
    parts, refs = refs[:n], refs[n:]
    if not first:
        (ml_in, a_in), refs = refs[:2], refs[2:]
        if not last:
            hm_in, refs = refs[0], refs[1:]
    if last:
        out_ref, k_all, ve = refs
    else:
        ml_ref, a_ref, hm_ref, k_all, ve = refs
    rows = q_ref.shape[0]
    pieces = pieces_of(parts, sources)
    tiles = [(at, min(TILE, total - at)) for at in range(0, total, TILE)]
    short = 16
    per_head = (rows, HEAD_SIZE)
    none = jnp.zeros(per_head, jnp.float32)

    def before(h, q):
        if not first:
            top = None if last else hm_in[h]
            return spread(ml_in[...], h), spread(ml_in[...], heads + h), a_in[h], top
        seen = lax.broadcasted_iota(jnp.int32, (rows, rows), 0) >= lax.broadcasted_iota(
            jnp.int32, (rows, rows), 1
        )
        s = jnp.where(seen, logits_of(q, own_ref[:, :HEAD_SIZE]), LOW)
        m = row_max(s)
        o = weigh(jnp.exp2(s - across(m, rows)), with_ones(own_ref[:, HEAD_SIZE:]))
        return m, o[:, HEAD_SIZE:], o[:, :HEAD_SIZE], by_sublane(m)

    def put(h, m, l, a, top, held):
        if last:
            out_ref[:, columns(h)] = (a / l).astype(out_ref.dtype)
            return held
        a_ref[h] = a
        hm_ref[h] = top
        held = jnp.where(lane_of(h, per_head), m, held)
        return jnp.where(lane_of(heads + h, per_head), l, held)

    def keep(held):
        if not last:
            ml_ref[...] = held

    def fast():
        gather(pieces, own_ref, k_all, ve)
        largest = jnp.full((8, HEAD_SIZE), LOW, jnp.float32)

        def head(h, carry):
            largest, held = carry
            q = q_ref[:, columns(h)]
            m, l, a, top = before(h, q)
            step = jnp.full(per_head, LOW, jnp.float32)
            o = None
            for start, size in tiles:
                d = logits_of(q, k_all[start : start + size]) - across(m, size)
                for j in range(0, size, HEAD_SIZE):
                    if j + HEAD_SIZE <= size:
                        step = jnp.maximum(step, d[:, j : j + HEAD_SIZE])
                    else:
                        step = jnp.maximum(step, row_max(d[:, j:]))
                pv = weigh(jnp.exp2(d), ve[start : start + size])
                o = pv if o is None else o + pv
            largest = jnp.maximum(largest, by_sublane(step))
            if not last:
                top = jnp.maximum(top, by_sublane(step + m))
            held = put(h, m, l + o[:, HEAD_SIZE:], a + o[:, :HEAD_SIZE], top, held)
            return largest, held

        carry = largest, none
        if at_once < heads:

            def some_heads(i, carry):
                for j in range(at_once):
                    carry = head(i * at_once + j, carry)
                return carry

            carry = lax.fori_loop(0, heads // at_once, some_heads, carry)
        else:
            for h in range(heads):
                carry = head(h, carry)
        largest, held = carry
        keep(held)

        @pl.when(jnp.max(largest) > LARGEST_STEP)
        def _():
            keep(lax.fori_loop(0, heads, again, none))

    def again(h, held):
        q = q_ref[:, columns(h)]
        m, l, a, top = before(h, q)

        def tile(i, state):
            m, l, a = state
            at = pl.ds(pl.multiple_of(i * short, short), short)
            s = logits_of(q, k_all[at])
            new = jnp.maximum(m, row_max(s))
            o = weigh(jnp.exp2(s - new[:, :short]), ve[at])
            kept = jnp.exp2(m - new)
            return new, l * kept + o[:, HEAD_SIZE:], a * kept + o[:, :HEAD_SIZE]

        m, l, a = lax.fori_loop(0, total // short, tile, (m, l, a))
        return put(h, m, l, a, None if last else jnp.maximum(top, by_sublane(m)), held)

    if first:
        fast()
        return
    some = pieces[0][-1]
    for piece in pieces[1:]:
        some = jnp.logical_or(some, piece[-1])

    @pl.when(jnp.logical_not(some))
    def _():
        def unchanged(h, held):
            return put(h, none, spread(ml_in[...], heads + h), a_in[h], None if last else hm_in[h], held)

        lax.fori_loop(0, heads, unchanged, none)
        if not last:
            keep(ml_in[...])

    pl.when(some)(fast)


def top_kernel(heads, sources, total, q_ref, own_ref, *refs):
    n = len(sources)
    parts, (hm_in, out_ref, k_all) = refs[:n], refs[n:]
    gather(pieces_of(parts, sources), own_ref, k_all, None)
    lane = lax.broadcasted_iota(jnp.int32, (1, heads), 1)
    tops = jnp.full((1, heads), LOW, jnp.float32)
    for h in range(heads):
        best = hm_in[h]
        for at in range(0, total, TILE):
            size = min(TILE, total - at)
            s = logits_of(q_ref[:, columns(h)], k_all[at : at + size])
            for j in range(0, size, HEAD_SIZE):
                if j + HEAD_SIZE <= size:
                    best = jnp.maximum(best, by_sublane(s[:, j : j + HEAD_SIZE]))
                else:
                    rest = row_max(s[:, j:])
                    best = jnp.maximum(best, by_sublane(rest))
        peak = jnp.max(jnp.max(best, axis=0, keepdims=True), axis=1, keepdims=True)
        tops = jnp.where(lane == h, peak * (1.0 / LOG2E), tops)
    out_ref[...] = jnp.broadcast_to(tops[None], out_ref.shape)


def cost(rows, heads, keys):
    return pl.CostEstimate(
        flops=4 * rows * heads * keys * HEAD_SIZE,
        bytes_accessed=2 * rows * heads * HEAD_SIZE,
        transcendentals=rows * heads * keys,
    )


def attend(q, kv, parts, sources, state, heads, at_once, last=False):
    rows = q.shape[0]
    total = sum(p.shape[0] for p in parts)
    first = state is None
    if last:
        out_shape = [jax.ShapeDtypeStruct(q.shape, jnp.bfloat16)]
    else:
        wide = jax.ShapeDtypeStruct((heads, rows, HEAD_SIZE), jnp.float32)
        thin = jax.ShapeDtypeStruct((rows, HEAD_SIZE), jnp.float32)
        out_shape = [thin, wide] + [jax.ShapeDtypeStruct((heads, 8, HEAD_SIZE), jnp.float32)]
    held = [] if first else list(state[:2] if last else state)
    return pl.pallas_call(
        lambda *refs: attend_kernel(heads, at_once, sources, total, first, last, *refs),
        out_shape=out_shape,
        in_specs=[VMEM] * (2 + len(parts) + len(held)),
        out_specs=[VMEM] * len(out_shape),
        scratch_shapes=[
            pltpu.VMEM((total, HEAD_SIZE), jnp.bfloat16),
            pltpu.VMEM((total, 2 * HEAD_SIZE), jnp.bfloat16),
        ],
        compiler_params=pltpu.CompilerParams(vmem_limit_bytes=VMEM_LIMIT),
        cost_estimate=cost(rows, heads, total + rows * first),
    )(q, kv, *parts, *held)


def local_tops(q, kv, parts, sources, hm, heads, devices):
    total = sum(p.shape[0] for p in parts)
    return pl.pallas_call(
        lambda *refs: top_kernel(heads, sources, total, *refs),
        out_shape=jax.ShapeDtypeStruct((devices, 1, heads), jnp.float32),
        in_specs=[VMEM] * (3 + len(parts)),
        out_specs=VMEM,
        scratch_shapes=[pltpu.VMEM((total, HEAD_SIZE), jnp.bfloat16)],
        compiler_params=pltpu.CompilerParams(vmem_limit_bytes=VMEM_LIMIT),
        cost_estimate=cost(q.shape[0], heads, total // 2),
    )(q, kv, *parts, hm)


def scale_kernel(everyones_ref, wq_ref, kw_ref, hm_ref, wq_out, kw_out):
    tp_size, heads = everyones_ref.shape[1:]
    maxima = jnp.max(everyones_ref[...], axis=0)
    mine = lax.broadcasted_iota(jnp.int32, maxima.shape, 0) == lax.axis_index("tp")
    own = jnp.max(jnp.where(mine, maxima, LOW), axis=0, keepdims=True)
    hm_ref[...] = own
    clip = CLIP_THRESHOLD / jnp.maximum(jnp.max(maxima, axis=1, keepdims=True), CLIP_THRESHOLD)
    own_clip = CLIP_THRESHOLD / jnp.maximum(jnp.max(own, axis=1, keepdims=True), CLIP_THRESHOLD)
    factor = CLIP_THRESHOLD / jnp.maximum(own, CLIP_THRESHOLD) / jnp.sqrt(own_clip)
    root = jnp.sqrt(clip)
    for h in range(heads):
        at = columns(h)
        wq_out[:, at] = (wq_ref[:, at].astype(jnp.float32) * factor[:, h : h + 1]).astype(wq_out.dtype)
    for g in range(tp_size):
        at = columns(g)
        kw_out[:, at] = (kw_ref[:, at].astype(jnp.float32) * root[g : g + 1]).astype(kw_out.dtype)


def scale_weights(everyones, w_query, key_weight):
    heads = everyones.shape[2]
    return pl.pallas_call(
        scale_kernel,
        out_shape=[
            jax.ShapeDtypeStruct((1, heads), jnp.float32),
            jax.ShapeDtypeStruct(w_query.shape, w_query.dtype),
            jax.ShapeDtypeStruct(key_weight.shape, key_weight.dtype),
        ],
        in_specs=[VMEM] * 3,
        out_specs=[VMEM] * 3,
        compiler_params=pltpu.CompilerParams(vmem_limit_bytes=VMEM_LIMIT),
        name="scale_weights",
    )(everyones, w_query, key_weight)


def shards(queries, keys, values, w_query, key_weight):
    heads = queries.shape[1] // HEAD_SIZE
    seq_size, tp_size = lax.axis_size("seq"), lax.axis_size("tp")
    zs = seq_size // X

    def moved(a, dz, dx):
        pairs = [
            (((z - dz) % zs) * X + (x - dx) % X, z * X + x) for z in range(zs) for x in range(X)
        ]
        return lax.ppermute(a, "seq", pairs)

    kv = jnp.concatenate([keys, values], axis=1)
    half_a, half_b = kv[:A_ROWS], kv[A_ROWS:]

    b_x = {dx: moved(half_b, 0, dx) for dx in (1, 3, 2)}
    along_z = [[z * X + x for z in range(zs)] for x in range(X)]
    column = lax.all_to_all(
        jnp.broadcast_to(half_a[None], (zs, *half_a.shape)),
        "seq",
        0,
        0,
        axis_index_groups=along_z,
        tiled=True,
    )
    column = column.reshape(zs * A_ROWS, kv.shape[1])
    layer = jnp.concatenate([half_b, b_x[1], b_x[2], b_x[3]], axis=0)
    b_up, b_down = [layer], [layer]
    for k in range(1, zs // 2 + 1):
        b_up.append(moved(b_up[-1], 1, 0))
        if k < zs // 2:
            b_down.append(moved(b_down[-1], -1, 0))
    a_x = {dx: moved(column, 0, dx) for dx in (1, 3, 2)}

    def b_part(k):
        return (b_up[k] if k > 0 else b_down[-k], [(k % zs, None, dx, zs) for dx in range(X)])

    def a_part(held, dx):
        return (held, [(None, z, dx, zs) for z in range(zs)])

    def more(state, parts, last=False, at_once=heads):
        parts, sources = zip(*parts) if parts else ((), ())
        return attend(queries, kv, parts, sources, state, heads, at_once, last)

    devices = seq_size * tp_size
    near = [(b_x[dx], [(0, None, dx, zs)]) for dx in (1, 2, 3)] + [a_part(column, 0)]
    late = [a_part(a_x[2], 2), b_part(4)]
    state = more(None, near)
    state = more(state, [b_part(1), b_part(-1)])
    state = more(state, [b_part(2), b_part(-2)])
    state = more(state, [a_part(a_x[1], 1)], at_once=heads // 2)
    state = more(state, [a_part(a_x[3], 3)])
    state = more(state, [b_part(3), b_part(-3)], at_once=heads // 2)
    tops = local_tops(queries, kv, *zip(*late), state[2], heads, devices)
    (attended,) = more(state, late, last=True, at_once=heads // 4)
    everyones = lax.all_to_all(tops, ("seq", "tp"), 0, 0, tiled=True)
    everyones = everyones.reshape(seq_size, tp_size, heads)
    head_max, w_query_clipped, clipped_key_weight = scale_weights(everyones, w_query, key_weight)
    return (attended, head_max.reshape(heads), w_query_clipped, clipped_key_weight)


def solution(mesh):
    in_specs = (P("seq", "tp"), P("seq", "tp"), P("seq", "tp"), P("seq", "tp"), P("seq", None))
    out_specs = (P("seq", "tp"), P("tp"), P("seq", "tp"), P("seq", None))

    return jax.shard_map(shards, mesh=mesh, in_specs=in_specs, out_specs=out_specs, check_vma=False)
```

```python
import jax
import jax.numpy as jnp
from jax import lax
from jax.experimental import pallas as pl
from jax.experimental.pallas import tpu as pltpu
from jax.sharding import PartitionSpec as P


HEAD_SIZE = 128
CLIP_THRESHOLD = 10.0
LOG2E = 1.4426950408889634
SCALE = HEAD_SIZE**-0.5 * LOG2E
LARGEST_STEP = 100.0
LOW = -1e30
X = 4
A_ROWS = 128
VMEM_LIMIT = 20 << 20
TILE = 1024
SLOW_ROWS = 64
SLOW_KEYS = 128


NT = (((1,), (1,)), ((), ()))
VMEM = pl.BlockSpec(memory_space=pltpu.VMEM)


def logits_of(q, k):
    return lax.dot_general(q, k, NT, preferred_element_type=jnp.float32) * SCALE


def weigh(p, ve):
    return jnp.dot(p.astype(jnp.bfloat16), ve, preferred_element_type=jnp.float32)


def with_ones(v):
    return jnp.concatenate([v, jnp.ones_like(v)], axis=1)


def across(column, width):
    wide = jnp.tile(column, (1, -(-width // column.shape[1])))
    return wide[:, :width]


def row_max(s):
    return jnp.broadcast_to(jnp.max(s, axis=1, keepdims=True), (s.shape[0], HEAD_SIZE))


def by_sublane(a):
    out = a[:8]
    for r in range(8, a.shape[0], 8):
        out = jnp.maximum(out, a[r : r + 8])
    return out


def columns(h):
    if isinstance(h, int):
        return pl.ds(h * HEAD_SIZE, HEAD_SIZE)
    return pl.ds(pl.multiple_of(h * HEAD_SIZE, HEAD_SIZE), HEAD_SIZE)


def pieces_of(refs, sources):
    place = lax.axis_index("seq")
    z, x = place // X, place % X
    base, found = 0, []
    for ref, source in zip(refs, sources):
        size = ref.shape[0] // len(source)
        for i, (dz, fixed_z, dx, zs) in enumerate(source):
            from_z = lax.rem(z + zs - dz, zs) if fixed_z is None else fixed_z
            came_from = from_z * X + lax.rem(x + X - dx, X)
            found.append((ref, i * size, base, size, came_from < place))
            base += size
    return found


def gather(pieces, own_ref, k_all, ve):
    first_key = own_ref[0:1, :HEAD_SIZE]
    for ref, start, base, size, earlier in pieces:
        rows = pl.ds(start, size)
        at = pl.ds(base, size)
        k_all[at] = jnp.where(
            earlier, ref[rows, :HEAD_SIZE], jnp.broadcast_to(first_key, (size, HEAD_SIZE))
        )
        if ve is not None:
            v = ref[rows, HEAD_SIZE:]
            ve[at, :HEAD_SIZE] = jnp.where(earlier, v, jnp.zeros_like(v))
            ve[at, HEAD_SIZE:] = jnp.where(earlier, jnp.ones_like(v), jnp.zeros_like(v))


def lane_of(h, shape):
    return lax.broadcasted_iota(jnp.int32, shape, 1) == h


def spread(per_head, h):
    if isinstance(h, int):
        return jnp.broadcast_to(per_head[:, h : h + 1], per_head.shape)
    return row_max(jnp.where(lane_of(h, per_head.shape), per_head, LOW))


def attend_kernel(heads, at_once, sources, total, first, last, q_ref, own_ref, *refs):
    n = len(sources)
    parts, refs = refs[:n], refs[n:]
    if not first:
        (ml_in, a_in), refs = refs[:2], refs[2:]
        if not last:
            hm_in, refs = refs[0], refs[1:]
    if last:
        out_ref, k_all, ve = refs
    else:
        ml_ref, a_ref, hm_ref, k_all, ve = refs
    rows = q_ref.shape[0]
    pieces = pieces_of(parts, sources)
    tiles = [(at, min(TILE, total - at)) for at in range(0, total, TILE)]
    per_head = (rows, HEAD_SIZE)
    none = jnp.zeros(per_head, jnp.float32)

    def before(h, q, r=0):
        n = q.shape[0]
        if not first:
            here = pl.ds(r, n)
            ml = ml_in[here]
            return spread(ml, h), spread(ml, heads + h), a_in[h, here]
        seen = r + lax.broadcasted_iota(jnp.int32, (n, rows), 0) >= lax.broadcasted_iota(
            jnp.int32, (n, rows), 1
        )
        s = jnp.where(seen, logits_of(q, own_ref[:, :HEAD_SIZE]), LOW)
        m = row_max(s)
        o = weigh(jnp.exp2(s - across(m, rows)), with_ones(own_ref[:, HEAD_SIZE:]))
        return m, o[:, HEAD_SIZE:], o[:, :HEAD_SIZE]

    def put(h, m, l, a, top, held):
        if last:
            out_ref[:, columns(h)] = (a / l).astype(out_ref.dtype)
            return held
        a_ref[h] = a
        hm_ref[h] = top
        held = jnp.where(lane_of(h, per_head), m, held)
        return jnp.where(lane_of(heads + h, per_head), l, held)

    def keep(held):
        if not last:
            ml_ref[...] = held

    def fast():
        gather(pieces, own_ref, k_all, ve)
        largest = jnp.full((8, HEAD_SIZE), LOW, jnp.float32)

        def head(h, carry):
            largest, held = carry
            q = q_ref[:, columns(h)]
            m, l, a = before(h, q)
            step = jnp.full(per_head, LOW, jnp.float32)
            o = None
            for start, size in tiles:
                d = logits_of(q, k_all[start : start + size]) - across(m, size)
                for j in range(0, size, HEAD_SIZE):
                    if j + HEAD_SIZE <= size:
                        step = jnp.maximum(step, d[:, j : j + HEAD_SIZE])
                    else:
                        step = jnp.maximum(step, row_max(d[:, j:]))
                pv = weigh(jnp.exp2(d), ve[start : start + size])
                o = pv if o is None else o + pv
            largest = jnp.maximum(largest, by_sublane(step))
            top = by_sublane(m if first else step + m)
            if first:
                top = jnp.maximum(top, by_sublane(step + m))
            elif not last:
                top = jnp.maximum(top, hm_in[h])
            held = put(h, m, l + o[:, HEAD_SIZE:], a + o[:, :HEAD_SIZE], top, held)
            return largest, held

        carry = largest, none
        if at_once < heads:

            def some_heads(i, carry):
                for j in range(at_once):
                    carry = head(i * at_once + j, carry)
                return carry

            carry = lax.fori_loop(0, heads // at_once, some_heads, carry)
        else:
            for h in range(heads):
                carry = head(h, carry)
        largest, held = carry
        keep(held)

        @pl.when(jnp.max(largest) > LARGEST_STEP)
        def _():
            lax.fori_loop(0, heads * (rows // SLOW_ROWS), again, 0)

    def again(i, carry):
        h = i // (rows // SLOW_ROWS)
        r = pl.multiple_of(i % (rows // SLOW_ROWS) * SLOW_ROWS, SLOW_ROWS)
        here = pl.ds(r, SLOW_ROWS)
        q = q_ref[here, columns(h)]

        def tile(j, state):
            m, l, a = state
            at = pl.ds(pl.multiple_of(j * SLOW_KEYS, SLOW_KEYS), SLOW_KEYS)
            s = logits_of(q, k_all[at])
            new = jnp.maximum(m, row_max(s))
            o = weigh(jnp.exp2(s - new), ve[at])
            kept = jnp.exp2(m - new)
            return new, l * kept + o[:, HEAD_SIZE:], a * kept + o[:, :HEAD_SIZE]

        m, l, a = lax.fori_loop(0, total // SLOW_KEYS, tile, before(h, q, r))
        if last:
            out_ref[here, columns(h)] = (a / l).astype(out_ref.dtype)
        else:
            a_ref[h, here] = a
            ml = jnp.where(lane_of(h, m.shape), m, ml_ref[here])
            ml_ref[here] = jnp.where(lane_of(heads + h, m.shape), l, ml)
        return carry

    if first:
        fast()
        return
    some = pieces[0][-1]
    for piece in pieces[1:]:
        some = jnp.logical_or(some, piece[-1])

    @pl.when(jnp.logical_not(some))
    def _():
        def unchanged(h, held):
            return put(h, none, spread(ml_in[...], heads + h), a_in[h], None if last else hm_in[h], held)

        lax.fori_loop(0, heads, unchanged, none)
        if not last:
            keep(ml_in[...])

    pl.when(some)(fast)


def top_kernel(heads, sources, total, q_ref, own_ref, *refs):
    n = len(sources)
    parts, (hm_in, out_ref, k_all) = refs[:n], refs[n:]
    gather(pieces_of(parts, sources), own_ref, k_all, None)
    lane = lax.broadcasted_iota(jnp.int32, (1, heads), 1)
    tops = jnp.full((1, heads), LOW, jnp.float32)
    for h in range(heads):
        best = hm_in[h]
        for at in range(0, total, TILE):
            size = min(TILE, total - at)
            s = logits_of(q_ref[:, columns(h)], k_all[at : at + size])
            for j in range(0, size, HEAD_SIZE):
                if j + HEAD_SIZE <= size:
                    best = jnp.maximum(best, by_sublane(s[:, j : j + HEAD_SIZE]))
                else:
                    rest = row_max(s[:, j:])
                    best = jnp.maximum(best, by_sublane(rest))
        peak = jnp.max(jnp.max(best, axis=0, keepdims=True), axis=1, keepdims=True)
        tops = jnp.where(lane == h, peak * (1.0 / LOG2E), tops)
    out_ref[...] = jnp.broadcast_to(tops[None], out_ref.shape)


def cost(rows, heads, keys):
    return pl.CostEstimate(
        flops=4 * rows * heads * keys * HEAD_SIZE,
        bytes_accessed=2 * rows * heads * HEAD_SIZE,
        transcendentals=rows * heads * keys,
    )


def attend(q, kv, parts, sources, state, heads, at_once, last=False):
    rows = q.shape[0]
    total = sum(p.shape[0] for p in parts)
    first = state is None
    if last:
        out_shape = [jax.ShapeDtypeStruct(q.shape, jnp.bfloat16)]
    else:
        wide = jax.ShapeDtypeStruct((heads, rows, HEAD_SIZE), jnp.float32)
        thin = jax.ShapeDtypeStruct((rows, HEAD_SIZE), jnp.float32)
        out_shape = [thin, wide] + [jax.ShapeDtypeStruct((heads, 8, HEAD_SIZE), jnp.float32)]
    held = [] if first else list(state[:2] if last else state)
    return pl.pallas_call(
        lambda *refs: attend_kernel(heads, at_once, sources, total, first, last, *refs),
        out_shape=out_shape,
        in_specs=[VMEM] * (2 + len(parts) + len(held)),
        out_specs=[VMEM] * len(out_shape),
        scratch_shapes=[
            pltpu.VMEM((total, HEAD_SIZE), jnp.bfloat16),
            pltpu.VMEM((total, 2 * HEAD_SIZE), jnp.bfloat16),
        ],
        compiler_params=pltpu.CompilerParams(vmem_limit_bytes=VMEM_LIMIT),
        cost_estimate=cost(rows, heads, total + rows * first),
    )(q, kv, *parts, *held)


def local_tops(q, kv, parts, sources, hm, heads, devices):
    total = sum(p.shape[0] for p in parts)
    return pl.pallas_call(
        lambda *refs: top_kernel(heads, sources, total, *refs),
        out_shape=jax.ShapeDtypeStruct((devices, 1, heads), jnp.float32),
        in_specs=[VMEM] * (3 + len(parts)),
        out_specs=VMEM,
        scratch_shapes=[pltpu.VMEM((total, HEAD_SIZE), jnp.bfloat16)],
        compiler_params=pltpu.CompilerParams(vmem_limit_bytes=VMEM_LIMIT),
        cost_estimate=cost(q.shape[0], heads, total // 2),
    )(q, kv, *parts, hm)


def scale_kernel(everyones_ref, wq_ref, kw_ref, hm_ref, wq_out, kw_out):
    tp_size, heads = everyones_ref.shape[1:]
    maxima = jnp.max(everyones_ref[...], axis=0)
    mine = lax.broadcasted_iota(jnp.int32, maxima.shape, 0) == lax.axis_index("tp")
    own = jnp.max(jnp.where(mine, maxima, LOW), axis=0, keepdims=True)
    hm_ref[...] = own
    clip = CLIP_THRESHOLD / jnp.maximum(jnp.max(maxima, axis=1, keepdims=True), CLIP_THRESHOLD)
    own_clip = CLIP_THRESHOLD / jnp.maximum(jnp.max(own, axis=1, keepdims=True), CLIP_THRESHOLD)
    factor = CLIP_THRESHOLD / jnp.maximum(own, CLIP_THRESHOLD) / jnp.sqrt(own_clip)
    root = jnp.sqrt(clip)
    for h in range(heads):
        at = columns(h)
        wq_out[:, at] = (wq_ref[:, at].astype(jnp.float32) * factor[:, h : h + 1]).astype(wq_out.dtype)
    for g in range(tp_size):
        at = columns(g)
        kw_out[:, at] = (kw_ref[:, at].astype(jnp.float32) * root[g : g + 1]).astype(kw_out.dtype)


def scale_weights(everyones, w_query, key_weight):
    heads = everyones.shape[2]
    return pl.pallas_call(
        scale_kernel,
        out_shape=[
            jax.ShapeDtypeStruct((1, heads), jnp.float32),
            jax.ShapeDtypeStruct(w_query.shape, w_query.dtype),
            jax.ShapeDtypeStruct(key_weight.shape, key_weight.dtype),
        ],
        in_specs=[VMEM] * 3,
        out_specs=[VMEM] * 3,
        compiler_params=pltpu.CompilerParams(vmem_limit_bytes=VMEM_LIMIT),
        name="scale_weights",
    )(everyones, w_query, key_weight)


def shards(queries, keys, values, w_query, key_weight):
    heads = queries.shape[1] // HEAD_SIZE
    seq_size, tp_size = lax.axis_size("seq"), lax.axis_size("tp")
    zs = seq_size // X

    def moved(a, dz, dx):
        pairs = [
            (((z - dz) % zs) * X + (x - dx) % X, z * X + x) for z in range(zs) for x in range(X)
        ]
        return lax.ppermute(a, "seq", pairs)

    kv = jnp.concatenate([keys, values], axis=1)
    half_a, half_b = kv[:A_ROWS], kv[A_ROWS:]

    b_x = {dx: moved(half_b, 0, dx) for dx in (1, 3, 2)}
    along_z = [[z * X + x for z in range(zs)] for x in range(X)]
    column = lax.all_to_all(
        jnp.broadcast_to(half_a[None], (zs, *half_a.shape)),
        "seq",
        0,
        0,
        axis_index_groups=along_z,
        tiled=True,
    )
    column = column.reshape(zs * A_ROWS, kv.shape[1])
    layer = jnp.concatenate([half_b, b_x[1], b_x[2], b_x[3]], axis=0)
    b_up, b_down = [layer], [layer]
    for k in range(1, zs // 2 + 1):
        b_up.append(moved(b_up[-1], 1, 0))
        if k < zs // 2:
            b_down.append(moved(b_down[-1], -1, 0))
    a_x = {dx: moved(column, 0, dx) for dx in (1, 3, 2)}

    def b_part(k):
        return (b_up[k] if k > 0 else b_down[-k], [(k % zs, None, dx, zs) for dx in range(X)])

    def a_part(held, dx):
        return (held, [(None, z, dx, zs) for z in range(zs)])

    def more(state, parts, last=False, at_once=heads):
        parts, sources = zip(*parts) if parts else ((), ())
        return attend(queries, kv, parts, sources, state, heads, at_once, last)

    devices = seq_size * tp_size
    near = [(b_x[dx], [(0, None, dx, zs)]) for dx in (1, 2, 3)] + [a_part(column, 0)]
    late = [b_part(4)]
    state = more(None, near)
    state = more(state, [b_part(1), b_part(-1)])
    state = more(state, [b_part(2), b_part(-2)])
    state = more(state, [a_part(a_x[1], 1)])
    state = more(state, [a_part(a_x[3], 3)])
    state = more(state, [a_part(a_x[2], 2), b_part(3), b_part(-3)])
    tops = local_tops(queries, kv, *zip(*late), state[2], heads, devices)
    (attended,) = more(state, late, last=True, at_once=1)
    everyones = lax.all_to_all(tops, ("seq", "tp"), 0, 0, tiled=True)
    everyones = everyones.reshape(seq_size, tp_size, heads)
    head_max, w_query_clipped, clipped_key_weight = scale_weights(everyones, w_query, key_weight)
    return (attended, head_max.reshape(heads), w_query_clipped, clipped_key_weight)


def solution(mesh):
    in_specs = (P("seq", "tp"), P("seq", "tp"), P("seq", "tp"), P("seq", "tp"), P("seq", None))
    out_specs = (P("seq", "tp"), P("tp"), P("seq", "tp"), P("seq", None))

    return jax.shard_map(shards, mesh=mesh, in_specs=in_specs, out_specs=out_specs, check_vma=False)
```

```python
import jax
import jax.numpy as jnp
from jax import lax
from jax.experimental import pallas as pl
from jax.experimental.pallas import tpu as pltpu
from jax.sharding import PartitionSpec as P


HEAD_SIZE = 128
CLIP_THRESHOLD = 10.0
LOG2E = 1.4426950408889634
SCALE = HEAD_SIZE**-0.5 * LOG2E
LARGEST_STEP = 100.0
LOW = -1e30
X = 4
A_ROWS = 128
VMEM_LIMIT = 20 << 20
TILE = 1024
SLOW_ROWS = 64
SLOW_KEYS = 128


NT = (((1,), (1,)), ((), ()))
VMEM = pl.BlockSpec(memory_space=pltpu.VMEM)


def logits_of(q, k):
    return lax.dot_general(q, k, NT, preferred_element_type=jnp.float32) * SCALE


def weigh(p, ve):
    return jnp.dot(p.astype(jnp.bfloat16), ve, preferred_element_type=jnp.float32)


def with_ones(v):
    return jnp.concatenate([v, jnp.ones_like(v)], axis=1)


def across(column, width):
    wide = jnp.tile(column, (1, -(-width // column.shape[1])))
    return wide[:, :width]


def row_max(s):
    return jnp.broadcast_to(jnp.max(s, axis=1, keepdims=True), (s.shape[0], HEAD_SIZE))


def by_sublane(a):
    out = a[:8]
    for r in range(8, a.shape[0], 8):
        out = jnp.maximum(out, a[r : r + 8])
    return out


def columns(h):
    if isinstance(h, int):
        return pl.ds(h * HEAD_SIZE, HEAD_SIZE)
    return pl.ds(pl.multiple_of(h * HEAD_SIZE, HEAD_SIZE), HEAD_SIZE)


def pieces_of(refs, sources):
    place = lax.axis_index("seq")
    z, x = place // X, place % X
    base, found = 0, []
    for ref, source in zip(refs, sources):
        size = ref.shape[0] // len(source)
        for i, (dz, fixed_z, dx, zs) in enumerate(source):
            from_z = lax.rem(z + zs - dz, zs) if fixed_z is None else fixed_z
            came_from = from_z * X + lax.rem(x + X - dx, X)
            found.append((ref, i * size, base, size, came_from < place))
            base += size
    return found


def gather(pieces, own_ref, k_all, ve):
    first_key = own_ref[0:1, :HEAD_SIZE]
    for ref, start, base, size, earlier in pieces:
        rows = pl.ds(start, size)
        at = pl.ds(base, size)
        k_all[at] = jnp.where(
            earlier, ref[rows, :HEAD_SIZE], jnp.broadcast_to(first_key, (size, HEAD_SIZE))
        )
        if ve is not None:
            v = ref[rows, HEAD_SIZE:]
            ve[at, :HEAD_SIZE] = jnp.where(earlier, v, jnp.zeros_like(v))
            ve[at, HEAD_SIZE:] = jnp.where(earlier, jnp.ones_like(v), jnp.zeros_like(v))


def lane_of(h, shape):
    return lax.broadcasted_iota(jnp.int32, shape, 1) == h


def spread(per_head, h):
    if isinstance(h, int):
        return jnp.broadcast_to(per_head[:, h : h + 1], per_head.shape)
    return row_max(jnp.where(lane_of(h, per_head.shape), per_head, LOW))


def attend_kernel(heads, at_once, sources, total, first, last, q_ref, own_ref, *refs):
    n = len(sources)
    parts, refs = refs[:n], refs[n:]
    if not first:
        (ml_in, a_in), refs = refs[:2], refs[2:]
        if not last:
            hm_in, refs = refs[0], refs[1:]
    if last:
        out_ref, k_all, ve = refs
    else:
        ml_ref, a_ref, hm_ref, k_all, ve = refs
    rows = q_ref.shape[0]
    pieces = pieces_of(parts, sources)
    tiles = [(at, min(TILE, total - at)) for at in range(0, total, TILE)]
    per_head = (rows, HEAD_SIZE)
    none = jnp.zeros(per_head, jnp.float32)

    def before(h, q, r=0):
        n = q.shape[0]
        if not first:
            here = pl.ds(r, n)
            ml = ml_in[here]
            return spread(ml, h), spread(ml, heads + h), a_in[h, here]
        seen = r + lax.broadcasted_iota(jnp.int32, (n, rows), 0) >= lax.broadcasted_iota(
            jnp.int32, (n, rows), 1
        )
        s = jnp.where(seen, logits_of(q, own_ref[:, :HEAD_SIZE]), LOW)
        m = row_max(s)
        o = weigh(jnp.exp2(s - across(m, rows)), with_ones(own_ref[:, HEAD_SIZE:]))
        return m, o[:, HEAD_SIZE:], o[:, :HEAD_SIZE]

    def put(h, m, l, a, top, held):
        if last:
            out_ref[:, columns(h)] = (a / l).astype(out_ref.dtype)
            return held
        a_ref[h] = a
        hm_ref[h] = top
        held = jnp.where(lane_of(h, per_head), m, held)
        return jnp.where(lane_of(heads + h, per_head), l, held)

    def keep(held):
        if not last:
            ml_ref[...] = held

    def fast():
        gather(pieces, own_ref, k_all, ve)
        largest = jnp.full((8, HEAD_SIZE), LOW, jnp.float32)

        def head(h, carry):
            largest, held = carry
            q = q_ref[:, columns(h)]
            m, l, a = before(h, q)
            step = jnp.full(per_head, LOW, jnp.float32)
            o = None
            for start, size in tiles:
                d = logits_of(q, k_all[start : start + size]) - across(m, size)
                for j in range(0, size, HEAD_SIZE):
                    if j + HEAD_SIZE <= size:
                        step = jnp.maximum(step, d[:, j : j + HEAD_SIZE])
                    else:
                        step = jnp.maximum(step, row_max(d[:, j:]))
                pv = weigh(jnp.exp2(d), ve[start : start + size])
                o = pv if o is None else o + pv
            largest = jnp.maximum(largest, by_sublane(step))
            top = by_sublane(m if first else step + m)
            if first:
                top = jnp.maximum(top, by_sublane(step + m))
            elif not last:
                top = jnp.maximum(top, hm_in[h])
            held = put(h, m, l + o[:, HEAD_SIZE:], a + o[:, :HEAD_SIZE], top, held)
            return largest, held

        carry = largest, none
        if at_once < heads:

            def some_heads(i, carry):
                for j in range(at_once):
                    carry = head(i * at_once + j, carry)
                return carry

            carry = lax.fori_loop(0, heads // at_once, some_heads, carry)
        else:
            for h in range(heads):
                carry = head(h, carry)
        largest, held = carry
        keep(held)

        @pl.when(jnp.max(largest) > LARGEST_STEP)
        def _():
            lax.fori_loop(0, heads * (rows // SLOW_ROWS), again, 0)

    def again(i, carry):
        h = i // (rows // SLOW_ROWS)
        r = pl.multiple_of(i % (rows // SLOW_ROWS) * SLOW_ROWS, SLOW_ROWS)
        here = pl.ds(r, SLOW_ROWS)
        q = q_ref[here, columns(h)]

        def tile(j, state):
            m, l, a = state
            at = pl.ds(pl.multiple_of(j * SLOW_KEYS, SLOW_KEYS), SLOW_KEYS)
            s = logits_of(q, k_all[at])
            new = jnp.maximum(m, row_max(s))
            o = weigh(jnp.exp2(s - new), ve[at])
            kept = jnp.exp2(m - new)
            return new, l * kept + o[:, HEAD_SIZE:], a * kept + o[:, :HEAD_SIZE]

        m, l, a = lax.fori_loop(0, total // SLOW_KEYS, tile, before(h, q, r))
        if last:
            out_ref[here, columns(h)] = (a / l).astype(out_ref.dtype)
        else:
            a_ref[h, here] = a
            ml = jnp.where(lane_of(h, m.shape), m, ml_ref[here])
            ml_ref[here] = jnp.where(lane_of(heads + h, m.shape), l, ml)
        return carry

    if first:
        fast()
        return
    some = pieces[0][-1]
    for piece in pieces[1:]:
        some = jnp.logical_or(some, piece[-1])

    @pl.when(jnp.logical_not(some))
    def _():
        def unchanged(h, held):
            return put(h, none, spread(ml_in[...], heads + h), a_in[h], None if last else hm_in[h], held)

        lax.fori_loop(0, heads, unchanged, none)
        if not last:
            keep(ml_in[...])

    pl.when(some)(fast)


def top_kernel(heads, sources, total, q_ref, own_ref, *refs):
    n = len(sources)
    parts, (hm_in, out_ref, k_all) = refs[:n], refs[n:]
    gather(pieces_of(parts, sources), own_ref, k_all, None)
    lane = lax.broadcasted_iota(jnp.int32, (1, heads), 1)
    tops = jnp.full((1, heads), LOW, jnp.float32)
    for h in range(heads):
        best = hm_in[h]
        for at in range(0, total, TILE):
            size = min(TILE, total - at)
            s = logits_of(q_ref[:, columns(h)], k_all[at : at + size])
            for j in range(0, size, HEAD_SIZE):
                if j + HEAD_SIZE <= size:
                    best = jnp.maximum(best, by_sublane(s[:, j : j + HEAD_SIZE]))
                else:
                    rest = row_max(s[:, j:])
                    best = jnp.maximum(best, by_sublane(rest))
        peak = jnp.max(jnp.max(best, axis=0, keepdims=True), axis=1, keepdims=True)
        tops = jnp.where(lane == h, peak * (1.0 / LOG2E), tops)
    out_ref[...] = jnp.broadcast_to(tops[None], out_ref.shape)


def cost(rows, heads, keys):
    return pl.CostEstimate(
        flops=4 * rows * heads * keys * HEAD_SIZE,
        bytes_accessed=2 * rows * heads * HEAD_SIZE,
        transcendentals=rows * heads * keys,
    )


def attend(q, kv, parts, sources, state, heads, at_once, last=False):
    rows = q.shape[0]
    total = sum(p.shape[0] for p in parts)
    first = state is None
    if last:
        out_shape = [jax.ShapeDtypeStruct(q.shape, jnp.bfloat16)]
    else:
        wide = jax.ShapeDtypeStruct((heads, rows, HEAD_SIZE), jnp.float32)
        thin = jax.ShapeDtypeStruct((rows, HEAD_SIZE), jnp.float32)
        out_shape = [thin, wide] + [jax.ShapeDtypeStruct((heads, 8, HEAD_SIZE), jnp.float32)]
    held = [] if first else list(state[:2] if last else state)
    return pl.pallas_call(
        lambda *refs: attend_kernel(heads, at_once, sources, total, first, last, *refs),
        out_shape=out_shape,
        in_specs=[VMEM] * (2 + len(parts) + len(held)),
        out_specs=[VMEM] * len(out_shape),
        scratch_shapes=[
            pltpu.VMEM((total, HEAD_SIZE), jnp.bfloat16),
            pltpu.VMEM((total, 2 * HEAD_SIZE), jnp.bfloat16),
        ],
        compiler_params=pltpu.CompilerParams(vmem_limit_bytes=VMEM_LIMIT),
        cost_estimate=cost(rows, heads, total + rows * first),
    )(q, kv, *parts, *held)


def local_tops(q, kv, parts, sources, hm, heads, devices):
    total = sum(p.shape[0] for p in parts)
    return pl.pallas_call(
        lambda *refs: top_kernel(heads, sources, total, *refs),
        out_shape=jax.ShapeDtypeStruct((devices, 1, heads), jnp.float32),
        in_specs=[VMEM] * (3 + len(parts)),
        out_specs=VMEM,
        scratch_shapes=[pltpu.VMEM((total, HEAD_SIZE), jnp.bfloat16)],
        compiler_params=pltpu.CompilerParams(vmem_limit_bytes=VMEM_LIMIT),
        cost_estimate=cost(q.shape[0], heads, total // 2),
    )(q, kv, *parts, hm)


def scale_kernel(everyones_ref, wq_ref, kw_ref, hm_ref, wq_out, kw_out):
    tp_size, heads = everyones_ref.shape[1:]
    maxima = jnp.max(everyones_ref[...], axis=0)
    mine = lax.broadcasted_iota(jnp.int32, maxima.shape, 0) == lax.axis_index("tp")
    own = jnp.max(jnp.where(mine, maxima, LOW), axis=0, keepdims=True)
    hm_ref[...] = own
    clip = CLIP_THRESHOLD / jnp.maximum(jnp.max(maxima, axis=1, keepdims=True), CLIP_THRESHOLD)
    own_clip = CLIP_THRESHOLD / jnp.maximum(jnp.max(own, axis=1, keepdims=True), CLIP_THRESHOLD)
    factor = CLIP_THRESHOLD / jnp.maximum(own, CLIP_THRESHOLD) / jnp.sqrt(own_clip)
    root = jnp.sqrt(clip)
    for h in range(heads):
        at = columns(h)
        wq_out[:, at] = (wq_ref[:, at].astype(jnp.float32) * factor[:, h : h + 1]).astype(wq_out.dtype)
    for g in range(tp_size):
        at = columns(g)
        kw_out[:, at] = (kw_ref[:, at].astype(jnp.float32) * root[g : g + 1]).astype(kw_out.dtype)


def scale_weights(everyones, w_query, key_weight):
    heads = everyones.shape[2]
    return pl.pallas_call(
        scale_kernel,
        out_shape=[
            jax.ShapeDtypeStruct((1, heads), jnp.float32),
            jax.ShapeDtypeStruct(w_query.shape, w_query.dtype),
            jax.ShapeDtypeStruct(key_weight.shape, key_weight.dtype),
        ],
        in_specs=[VMEM] * 3,
        out_specs=[VMEM] * 3,
        compiler_params=pltpu.CompilerParams(vmem_limit_bytes=VMEM_LIMIT),
        name="scale_weights",
    )(everyones, w_query, key_weight)


def shards(queries, keys, values, w_query, key_weight):
    heads = queries.shape[1] // HEAD_SIZE
    seq_size, tp_size = lax.axis_size("seq"), lax.axis_size("tp")
    zs = seq_size // X

    def moved(a, dz, dx):
        pairs = [
            (((z - dz) % zs) * X + (x - dx) % X, z * X + x) for z in range(zs) for x in range(X)
        ]
        return lax.ppermute(a, "seq", pairs)

    kv = jnp.concatenate([keys, values], axis=1)
    half_a, half_b = kv[:A_ROWS], kv[A_ROWS:]

    b_x = {dx: moved(half_b, 0, dx) for dx in (1, 3, 2)}
    along_z = [[z * X + x for z in range(zs)] for x in range(X)]
    column = lax.all_to_all(
        jnp.broadcast_to(half_a[None], (zs, *half_a.shape)),
        "seq",
        0,
        0,
        axis_index_groups=along_z,
        tiled=True,
    )
    column = column.reshape(zs * A_ROWS, kv.shape[1])
    layer = jnp.concatenate([half_b, b_x[1], b_x[2], b_x[3]], axis=0)
    b_up, b_down = [layer], [layer]
    for k in range(1, zs // 2 + 1):
        b_up.append(moved(b_up[-1], 1, 0))
        if k < zs // 2:
            b_down.append(moved(b_down[-1], -1, 0))
    a_x = {dx: moved(column, 0, dx) for dx in (1, 3, 2)}

    def b_part(k):
        return (b_up[k] if k > 0 else b_down[-k], [(k % zs, None, dx, zs) for dx in range(X)])

    def a_part(held, dx):
        return (held, [(None, z, dx, zs) for z in range(zs)])

    def more(state, parts, last=False, at_once=heads):
        parts, sources = zip(*parts) if parts else ((), ())
        return attend(queries, kv, parts, sources, state, heads, at_once, last)

    devices = seq_size * tp_size
    near = [(b_x[dx], [(0, None, dx, zs)]) for dx in (1, 2, 3)] + [a_part(column, 0)]
    late = [b_part(4), b_part(-3)]
    state = more(None, near)
    state = more(state, [b_part(1), b_part(-1)])
    state = more(state, [b_part(2), b_part(-2)])
    state = more(state, [a_part(a_x[1], 1)])
    state = more(state, [a_part(a_x[3], 3)])
    state = more(state, [a_part(a_x[2], 2), b_part(3)])
    tops = local_tops(queries, kv, *zip(*late), state[2], heads, devices)
    (attended,) = more(state, late, last=True, at_once=2)
    everyones = lax.all_to_all(tops, ("seq", "tp"), 0, 0, tiled=True)
    everyones = everyones.reshape(seq_size, tp_size, heads)
    head_max, w_query_clipped, clipped_key_weight = scale_weights(everyones, w_query, key_weight)
    return (attended, head_max.reshape(heads), w_query_clipped, clipped_key_weight)


def solution(mesh):
    in_specs = (P("seq", "tp"), P("seq", "tp"), P("seq", "tp"), P("seq", "tp"), P("seq", None))
    out_specs = (P("seq", "tp"), P("tp"), P("seq", "tp"), P("seq", None))

    return jax.shard_map(shards, mesh=mesh, in_specs=in_specs, out_specs=out_specs, check_vma=False)
```
